128 devices in a mesh: rows: 4 (over y_hi, core), cols: 32 (over y_lo, x, z).
Axes of the slice: x: 4, y: 4 (y_hi: 2, y_lo: 2; y = y_hi * 2 + y_lo), z: 4, core: 2. Of those that a mesh axis runs over, the one named last changes fastest.
Arguments:
- features: bfloat16 [131072, 2048], P(('rows', 'cols')), may hold values from -6 to 6
- w_in: bfloat16 [2048, 1024], replicated, may hold values from -0.125 to 0.125
- w_out: bfloat16 [1024, 256], replicated, may hold values from -0.1875 to 0.1875
- item_ids: int32 [131072], P(('rows', 'cols')), may hold values from 0 to 131071, as said below
- item_counts: int32 [131072], P(('rows', 'cols')), may hold values from 0 to 65535
- owners: int32 [131072, 1], P(('rows', 'cols')), may hold values from 0 to 127; in each aligned block of 1024 rows (0 to 1023, 1024 to 2047, ...) at most 16 rows name the same one
- queries: bfloat16 [8192, 256], P('rows'), may hold values from -60 to 60
- positives: int32 [8192], replicated, may hold values from 0 to 131071, as said below
Outputs:
- cache_emb: bfloat16 [262144, 256], P(('rows', 'cols'))
- cache_ids: int32 [262144], P(('rows', 'cols'))
- query_loss: float32 [8192], P('rows')
The draws below stay inside these ranges and needn't reach their ends.
Inputs may be any that keep to these rules, and one draw needn't show every extreme that they name: `item_ids`: all ids are different. `owners`: the items of one device name each owner at most 16 times; some owner is named exactly 16 times by one device's items. `positives`: each is the id of some item.
All inputs are finite; a program needn't handle non-finite values.
Results may differ from the reference program's by a relative error of at most 0.0049.
Values may be sent and summed in bfloat16 or wider, within the bound.
No kernel may reach another device: no remote copies, remote signals or barrier semaphores. Data moves between devices by JAX's collectives and lax.ppermute only.
A program may use at most 128 MiB of HBM per device.

```python
import math
import jax
import jax.numpy as jnp
import numpy as np
from jax import lax

F_IN = 2048
HID = 1024
EMB = 256
ITEMS_DEV = 1024
ITEMS = 131072
CAP = 16
QUERIES = 8192
POOL = 262144
DEVICES = 128


def shared_ids(key):
    return jax.random.permutation(jax.random.fold_in(key, 29), ITEMS).astype(jnp.int32)


def draw_item_ids(key, part):
    return shared_ids(key)


def draw_positives(key, part):
    identity = shared_ids(key)
    key_order, key_offset = jax.random.split(jax.random.fold_in(key, 31), 2)
    blocks = QUERIES // DEVICES
    scores = jax.random.randint(key_order, (blocks, DEVICES), 0, 1 << 20) * DEVICES + jnp.arange(DEVICES, dtype=jnp.int32)[None, :]
    producer = jnp.argsort(scores, axis=1, stable=True).astype(jnp.int32).reshape(QUERIES)
    offset = jax.random.randint(key_offset, (QUERIES,), 0, ITEMS_DEV).astype(jnp.int32)
    return identity[producer * ITEMS_DEV + offset].astype(jnp.int32)


def draw_queries(key, part):
    key_base = jax.random.fold_in(jax.random.fold_in(key, 17), 0)
    values = jax.random.normal(key_base, (QUERIES, EMB), jnp.float32)
    return jnp.clip(values, -6.0, 6.0).astype(jnp.bfloat16)


def place_ends(drawn, stream_key, low, top_value):
    shape = drawn.shape
    place = [jax.random.randint(jax.random.fold_in(stream_key, axis), (), 0, shape[axis]) for axis in range(len(shape))]
    drawn = drawn.at[tuple(place)].set(low)
    longest = shape.index(max(shape))
    place[longest] = (place[longest] + 1) % shape[longest]
    return drawn.at[tuple(place)].set(top_value)


def block_levels(key, dims, pieces, smallest, largest):
    gain = 1.0
    for position, parts in pieces:
        draws = jax.random.uniform(jax.random.fold_in(jax.random.fold_in(key, 6), position), (parts,), jnp.float32, smallest / len(pieces), largest / len(pieces))
        gain = gain * jnp.repeat(jnp.exp(draws), dims[position] // parts).reshape((-1,) + (1,) * (len(dims) - 1 - position))
    return gain


def rank_table(count, slope):
    portions = [(1 << 20) // math.isqrt(standing ** slope) + 1 for standing in range(1, count + 1)]
    deviation = 1 + sum(portions) // (1 << 30)
    return np.cumsum(np.array([max(1, weight // deviation) for weight in portions]))


def ranked(stream_key, dims, count, skew):
    table = rank_table(count, skew)
    lot = jax.random.randint(jax.random.fold_in(stream_key, 1), dims, 0, int(table[count - 1]))
    rank = jnp.searchsorted(jnp.asarray(table, jnp.int32), lot, side="right")
    return jax.random.permutation(jax.random.fold_in(stream_key, 2), count)[rank].astype(jnp.int32)


def assign_block(rng, own, number, rows, amount, top, most, slope):
    order = jax.random.permutation(rng, amount)
    packed, common = shares(amount, rows * top, most, slope, True), shares(amount, rows * top, most, slope, False)
    places = jnp.arange(amount)

    def named(tallies, rotation):
        used = int((tallies > 0).sum())
        fixed = max(1, used // 4)
        passed = fixed + (places - fixed + rotation * (used - fixed)) % max(1, amount - fixed)
        return jnp.zeros((amount,), jnp.int32).at[order[jnp.where(places < fixed, places, passed)]].set(jnp.asarray(tallies, jnp.int32))

    tallies = jnp.where(number % 4 == 0, named(packed, number // 4), named(common, number - number // 4 - 1))
    mixed = jax.random.permutation(jax.random.fold_in(own, 3), amount)
    source_of, taker = mixed[0:amount // 2 * 2:2], mixed[1:amount // 2 * 2:2]
    room = jnp.minimum(tallies[source_of] - 1, most - tallies[taker]) // 2
    room = jnp.where((source_of == order[0]) | (taker == order[0]) | (tallies[taker] == 0), 0, jnp.maximum(room, 0))
    passed = jax.random.randint(jax.random.fold_in(own, 4), (amount // 2,), 0, 1 << 20) % (room + 1)
    tallies = tallies.at[source_of].add(-passed).at[taker].add(passed)
    items = jnp.searchsorted(jnp.cumsum(tallies), jnp.arange(rows * top), side="right").astype(jnp.int32)
    listing = items.reshape(top, rows).T
    listing = listing[jax.random.permutation(jax.random.fold_in(own, 1), rows)]
    rotation = jax.random.randint(jax.random.fold_in(own, 2), (rows, 1), 0, top)
    return jnp.take_along_axis(listing, (jnp.arange(top)[None, :] + rotation) % top, axis=1)


def shares(number_of, total, most, skew, full):
    loads = [(1 << 20) // math.isqrt(rank ** skew) + 1 for rank in range(1, number_of + 1)]
    largest = most if full else min(most, max(-(-total // number_of), total * loads[0] // sum(loads)))
    least = 1 if total - largest >= number_of - 1 else 0
    given, spare = [largest] + [least] * (number_of - 1), total - largest - least * (number_of - 1)
    while spare > 0:
        movable = [i for i in range(1, number_of) if given[i] < largest] or [i for i in range(1, number_of) if given[i] < most]
        pool, left = sum([loads[i] for i in movable]), spare
        for i in movable:
            more = min(most - given[i], max(1, left * loads[i] // pool), spare)
            given[i] = given[i] + more
            spare = spare - more
    return np.array(given)


def normal_values(stream_key, extent, spread, reach, cuts=(), held_as=jnp.bfloat16):
    entries = jax.random.normal(stream_key, extent, jnp.float32) * spread
    if len(cuts) > 0:
        entries = block_levels(stream_key, extent, cuts, -0.22, 0.18) * entries
    return jnp.clip(entries, min=-reach, max=reach).astype(held_as)


def setup_inputs(seed: int = 0) -> dict:
    key_of = jax.random.split(jax.random.key(seed), 9)
    features = normal_values(key_of[0], (ITEMS, F_IN), 1.0, 6.0, ((0, 128),))
    w_in = normal_values(key_of[1], (F_IN, HID), F_IN ** -0.5, 0.125)
    w_out = normal_values(key_of[2], (HID, EMB), HID ** -0.5, 0.1875)
    item_ids = draw_item_ids(jax.random.fold_in(key_of[8], 71), 0)
    item_counts = place_ends(ranked(key_of[4], (ITEMS,), 65536, 2), jax.random.fold_in(key_of[4], 3), 0, 65535).astype(jnp.int32)
    owners_keys = jax.random.split(jax.random.fold_in(key_of[5], 1), ITEMS // ITEMS_DEV)
    owners_turns = jax.random.permutation(jax.random.fold_in(key_of[5], 3), ITEMS // ITEMS_DEV)
    owners = jax.vmap(lambda own, number: assign_block(jax.random.fold_in(key_of[5], 2), own, number, ITEMS_DEV, DEVICES, 1, CAP, 1))(owners_keys, owners_turns).reshape((ITEMS, 1))
    queries = draw_queries(jax.random.fold_in(key_of[8], 71), 0)
    positives = draw_positives(jax.random.fold_in(key_of[8], 71), 0)
    return dict(features=features, w_in=w_in, w_out=w_out, item_ids=item_ids, item_counts=item_counts, owners=owners, queries=queries, positives=positives)


def item_tower(block_rows, w_in, w_out):
    hidden = jnp.maximum(jnp.dot(block_rows, w_in, preferred_element_type=jnp.float32), 0.0).astype(jnp.bfloat16)
    return jnp.dot(hidden, w_out, preferred_element_type=jnp.float32).astype(jnp.bfloat16)

def rank_rows(owner_row):
    onehot = (owner_row[:, None] == jnp.arange(DEVICES, dtype=jnp.int32)[None, :]).astype(jnp.int32)
    before = jnp.cumsum(onehot, axis=0) - onehot
    return lax.optimization_barrier(jnp.sum(before * onehot, axis=1)).astype(jnp.int32)

def reference(features, w_in, w_out, item_ids, item_counts, owners, queries, positives):

    def tower_block(block_rows):
        return item_tower(block_rows, w_in, w_out)
    embedded = lax.map(tower_block, features.reshape(DEVICES, ITEMS_DEV, F_IN)).reshape(ITEMS, EMB)
    owner_index = owners[:, 0].astype(jnp.int32)
    rank_within = lax.map(rank_rows, owner_index.reshape(DEVICES, ITEMS_DEV)).reshape(ITEMS)
    source = jnp.arange(ITEMS, dtype=jnp.int32) // ITEMS_DEV
    cache_index = (owner_index * (DEVICES * CAP) + source * CAP + rank_within).astype(jnp.int32)
    cache_emb = jnp.zeros((POOL, EMB), jnp.bfloat16).at[cache_index].set(embedded)
    cache_ids = jnp.full((POOL,), -1, jnp.int32).at[cache_index].set(item_ids)
    log_q = jnp.log1p(item_counts.astype(jnp.float32))
    score_scale = 4.0 / math.sqrt(EMB)
    row_of_id = jnp.zeros((ITEMS,), jnp.int32).at[item_ids.astype(jnp.int32)].set(jnp.arange(ITEMS, dtype=jnp.int32))
    pos_row = row_of_id[positives.astype(jnp.int32)].astype(jnp.int32)
    pos_emb = embedded[pos_row]
    pos_logit = lax.optimization_barrier(jnp.sum(queries.astype(jnp.float32) * pos_emb.astype(jnp.float32), axis=1)) * score_scale - log_q[pos_row]
    block_rows = min(QUERIES, 512)
    key_rows = embedded.T

    def block_lse(query_block):
        raw_scores = jnp.dot(query_block, key_rows, preferred_element_type=jnp.float32) * score_scale - log_q[None, :]
        highest = lax.optimization_barrier(jnp.max(raw_scores, axis=1, keepdims=True))
        return highest[:, 0] + jnp.log(lax.optimization_barrier(jnp.sum(jnp.exp(raw_scores - highest), axis=1)))
    log_total = lax.map(block_lse, queries.reshape(QUERIES // block_rows, block_rows, EMB)).reshape(QUERIES)
    query_loss = log_total - pos_logit
    return (cache_emb, cache_ids, query_loss)
```

```python
import math

import jax
import jax.numpy as jnp
from jax import lax
from jax.experimental import pallas as pl
from jax.experimental.pallas import tpu as pltpu
from jax.sharding import Mesh
from jax.sharding import PartitionSpec as P

ROWS = ("rows_0", "rows_1")
COLS = ("cols_0", "cols_1", "cols_2")
ROWS_COLS = ("rows_0", "rows_1", "cols_0", "cols_1", "cols_2")

F32 = jnp.float32
BF16 = jnp.bfloat16
I32 = jnp.int32

N_DEV = 128
N_ROWS = 4
N_COLS = 32
ITEMS = 1024
CAP = 16
EMB = 256
HID = 1024
F_IN = 2048
QDEV = 2048
LANES = 128
BLOCKS = ITEMS // LANES

LOG2E = math.log2(math.e)
LN2 = math.log(2.0)
SCALE2 = 4.0 / math.sqrt(EMB) * LOG2E
FLOOR = -1e30

PACK_IDS = N_DEV
PACK_LOGQ = N_DEV + BLOCKS
PACK_ROWS = N_DEV + 2 * BLOCKS

PART_POS = QDEV // LANES
PART_IDS = 2 * PART_POS
PART_ROWS = PART_IDS + 8

NT = (((1,), (1,)), ((), ()))

ROW_BLOCK = 256


def tower_kernel(
    feat_hbm, w_in_hbm, w_out_hbm, owners_ref, ids_ref, counts_ref,
    emb_ref, send_ref, pack_ref,
    feat, w_in, w_out, slots, feat_sem, w_in_sem, w_out_sem,
):
    n_blocks = ITEMS // ROW_BLOCK
    copies = [
        pltpu.make_async_copy(
            feat_hbm.at[pl.ds(k * ROW_BLOCK, ROW_BLOCK)],
            feat.at[pl.ds(k * ROW_BLOCK, ROW_BLOCK)],
            feat_sem.at[k],
        )
        for k in range(n_blocks)
    ]
    w_in_copy = pltpu.make_async_copy(w_in_hbm, w_in, w_in_sem)
    w_out_copy = pltpu.make_async_copy(w_out_hbm, w_out, w_out_sem)
    copies[0].start()
    w_in_copy.start()
    w_out_copy.start()
    for k in range(1, n_blocks):
        copies[k].start()

    owner_iota = lax.broadcasted_iota(I32, (N_DEV, LANES), 0)
    upper = (
        lax.broadcasted_iota(I32, (LANES, LANES), 0) < lax.broadcasted_iota(I32, (LANES, LANES), 1)
    ).astype(F32).astype(BF16)
    slot_of_lane = lax.broadcasted_iota(I32, (LANES, LANES), 0) % CAP
    seen = jnp.zeros((N_DEV, 1), F32)
    parts = [jnp.zeros((N_DEV, LANES), F32) for _ in range(3)]
    for j in range(BLOCKS):
        owner = owners_ref[j : j + 1, :]
        onehot = (owner_iota == owner).astype(F32)
        onehot_b = onehot.astype(BF16)
        before = jnp.dot(onehot_b, upper, preferred_element_type=F32) + seen
        rank = jnp.sum(onehot * before, axis=0, keepdims=True).astype(I32)
        seen = seen + jnp.sum(onehot, axis=1, keepdims=True)
        slots[j : j + 1, :] = owner * CAP + rank
        value = ids_ref[j : j + 1, :] + 1
        here = slot_of_lane == rank
        for p, piece in enumerate((value >> 12, (value >> 6) & 63, value & 63)):
            chosen = jnp.where(here, piece.astype(F32), 0.0).astype(BF16)
            parts[p] = parts[p] + lax.dot_general(onehot_b, chosen, NT, preferred_element_type=F32)
    pack_ref[0:N_DEV, :] = parts[0] * 4096.0 + parts[1] * 64.0 + parts[2] - 1.0
    pack_ref[PACK_IDS : PACK_IDS + BLOCKS, :] = ids_ref[...].astype(F32)
    pack_ref[PACK_LOGQ : PACK_LOGQ + BLOCKS, :] = jnp.log(1.0 + counts_ref[...].astype(F32)) * LOG2E

    for k in range(n_blocks):
        copies[k].wait()
        if k == 0:
            w_in_copy.wait()
        rows = pl.ds(k * ROW_BLOCK, ROW_BLOCK)
        hidden = jnp.maximum(
            jnp.dot(feat[rows, :], w_in[...], preferred_element_type=F32), 0.0
        ).astype(BF16)
        if k == 0:
            w_out_copy.wait()
        emb_ref[rows, :] = jnp.dot(hidden, w_out[...], preferred_element_type=F32).astype(BF16)

    chunk = 512
    slot_row = jnp.concatenate([slots[j : j + 1, :] for j in range(BLOCKS)], axis=1)
    for c in range(N_DEV * CAP // chunk):
        place = lax.broadcasted_iota(I32, (chunk, ITEMS), 0) + c * chunk
        chosen = (place == slot_row).astype(F32).astype(BF16)
        send_ref[pl.ds(c * chunk, chunk), :] = jnp.dot(
            chosen, emb_ref[...], preferred_element_type=F32
        ).astype(BF16)


def tower(features, w_in, w_out, owners, ids, counts):
    any_spec = pl.BlockSpec(memory_space=pl.ANY)
    vmem_spec = pl.BlockSpec(memory_space=pltpu.VMEM)
    n_blocks = ITEMS // ROW_BLOCK
    return pl.pallas_call(
        tower_kernel,
        in_specs=[any_spec, any_spec, any_spec, vmem_spec, vmem_spec, vmem_spec],
        out_specs=[vmem_spec, vmem_spec, vmem_spec],
        out_shape=[
            jax.ShapeDtypeStruct((ITEMS, EMB), BF16),
            jax.ShapeDtypeStruct((N_DEV * CAP, EMB), BF16),
            jax.ShapeDtypeStruct((PACK_ROWS, LANES), F32),
        ],
        scratch_shapes=[
            pltpu.VMEM((ITEMS, F_IN), BF16),
            pltpu.VMEM((F_IN, HID), BF16),
            pltpu.VMEM((HID, EMB), BF16),
            pltpu.VMEM((BLOCKS, LANES), I32),
            pltpu.SemaphoreType.DMA((n_blocks,)),
            pltpu.SemaphoreType.DMA,
            pltpu.SemaphoreType.DMA,
        ],
        cost_estimate=pl.CostEstimate(
            flops=2 * ITEMS * F_IN * HID + 2 * ITEMS * HID * EMB,
            bytes_accessed=2 * (ITEMS * F_IN + F_IN * HID),
            transcendentals=0,
        ),
        name="tower",
    )(features, w_in, w_out, owners, ids, counts)


Q_TILE = 256
I_TILE = 512


def score_blocks(q_ref, pos_ref, embs, packs, col_ids, col_logq, state_in, state_out):
    for n, pack in enumerate(packs):
        for rows, col in ((PACK_IDS, col_ids), (PACK_LOGQ, col_logq)):
            turned = jnp.concatenate(
                [pack[pl.ds(rows, BLOCKS), :], jnp.zeros((LANES - BLOCKS, LANES), F32)], axis=0
            ).T
            for j in range(BLOCKS):
                col[pl.ds(n * ITEMS + j * LANES, LANES), :] = jnp.broadcast_to(
                    turned[:, j : j + 1], (LANES, LANES)
                )

    def query_tile(t, _):
        q_rows = q_ref[pl.ds(pl.multiple_of(t * Q_TILE, Q_TILE), Q_TILE), :]
        pos_rows = [
            pos_ref[pl.ds(t * (Q_TILE // LANES) + u, 1), :].astype(F32) for u in range(Q_TILE // LANES)
        ]
        pos_row = jnp.concatenate(pos_rows, axis=1)
        top, total, hit = [state_in(k, t) for k in range(3)]
        for n, emb in enumerate(embs):
            for c in range(ITEMS // I_TILE):
                raw = lax.dot_general(
                    emb[pl.ds(c * I_TILE, I_TILE), :], q_rows, NT, preferred_element_type=F32
                )
                at = pl.ds(n * ITEMS + c * I_TILE, I_TILE)
                logq = jnp.concatenate([col_logq[at, :]] * (Q_TILE // LANES), axis=1)
                ids = jnp.concatenate([col_ids[at, :]] * (Q_TILE // LANES), axis=1)
                logit = raw * SCALE2 - logq
                match = jnp.where(ids == pos_row, logit, 0.0)
                grouped = logit.reshape(I_TILE // 8, 8, Q_TILE)
                new_top = jnp.maximum(top, jnp.max(grouped, axis=0))
                total = total * jnp.exp2(top - new_top) + jnp.sum(
                    jnp.exp2(grouped - new_top[None]), axis=0
                )
                hit = hit + jnp.sum(match.reshape(I_TILE // 8, 8, Q_TILE), axis=0)
                top = new_top
        state_out(t, top, total, hit)
        return 0

    lax.fori_loop(0, QDEV // Q_TILE, query_tile, 0)


def near_kernel(
    where_ref, q_ref, pos_all, emb0, emb1, pack0, pack1, state_ref, col_ids, col_logq
):
    pos_ref = pos_all.at[pl.ds(where_ref[0] * (QDEV // LANES), QDEV // LANES)]

    def state_in(k, t):
        return jnp.full((8, Q_TILE), FLOOR if k == 0 else 0.0, F32)

    def state_out(t, *state):
        for k in range(3):
            state_ref[k, t] = state[k]

    score_blocks(q_ref, pos_ref, (emb0, emb1), (pack0, pack1), col_ids, col_logq, state_in, state_out)


def far_kernel(
    where_ref, q_ref, pos_all, emb0, emb1, pack0, pack1, near0, near1, before_ref,
    out_ref, parts, col_ids, col_logq,
):
    row = where_ref[0]
    col = where_ref[1]
    pos_ref = pos_all.at[pl.ds(row * (QDEV // LANES), QDEV // LANES)]

    def state_in(k, t):
        return before_ref[k, t]

    def state_out(t, top, total, hit):
        highest = jnp.max(top, axis=0, keepdims=True)
        summed = jnp.sum(total * jnp.exp2(top - highest), axis=0, keepdims=True)
        both = (highest + jnp.log(summed) * LOG2E, jnp.sum(hit, axis=0, keepdims=True))
        for k in range(2):
            for u in range(Q_TILE // LANES):
                parts[pl.ds(k * PART_POS + t * (Q_TILE // LANES) + u, 1), :] = both[k][
                    :, u * LANES : (u + 1) * LANES
                ]

    score_blocks(q_ref, pos_ref, (emb0, emb1), (pack0, pack1), col_ids, col_logq, state_in, state_out)

    out_ref[:, 0:PART_IDS, :] = jnp.broadcast_to(
        parts[...][None], (N_COLS, PART_IDS, LANES)
    )
    mine = lax.broadcasted_iota(I32, (N_COLS, 8, LANES), 2) // CAP == col % 8
    place = lax.broadcasted_iota(I32, (N_COLS, 8, LANES), 1)
    rows = pl.ds(row * N_COLS, N_COLS)
    found = jnp.zeros((N_COLS, 8, LANES), F32)
    for source, pack in (
        (row, near0), (row ^ 1, near1), (row ^ 2, pack0), (row ^ 3, pack1)
    ):
        found = jnp.where(
            mine & (place == source),
            jnp.broadcast_to(pack[rows, :][:, None, :], (N_COLS, 8, LANES)),
            found,
        )
    out_ref[:, PART_IDS:PART_ROWS, :] = found


SCORE_COST = pl.CostEstimate(
    flops=2 * QDEV * 2 * ITEMS * EMB,
    bytes_accessed=2 * (QDEV * EMB + 2 * ITEMS * EMB),
    transcendentals=QDEV * 2 * ITEMS,
)


def score_near(where, queries, pos, embs, packs):
    vmem_spec = pl.BlockSpec(memory_space=pltpu.VMEM)
    return pl.pallas_call(
        near_kernel,
        in_specs=[pl.BlockSpec(memory_space=pltpu.SMEM)] + [vmem_spec] * 6,
        out_specs=vmem_spec,
        out_shape=jax.ShapeDtypeStruct((3, QDEV // Q_TILE, 8, Q_TILE), F32),
        scratch_shapes=[pltpu.VMEM((2 * ITEMS, LANES), F32)] * 2,
        cost_estimate=SCORE_COST,
        name="score_near",
    )(where, queries, pos, *embs, *packs)


def score_far(where, queries, pos, embs, packs, near_packs, state):
    vmem_spec = pl.BlockSpec(memory_space=pltpu.VMEM)
    return pl.pallas_call(
        far_kernel,
        in_specs=[pl.BlockSpec(memory_space=pltpu.SMEM)] + [vmem_spec] * 9,
        out_specs=vmem_spec,
        out_shape=jax.ShapeDtypeStruct((N_COLS, PART_ROWS, LANES), F32),
        scratch_shapes=[pltpu.VMEM((PART_IDS, LANES), F32)]
        + [pltpu.VMEM((2 * ITEMS, LANES), F32)] * 2,
        cost_estimate=SCORE_COST,
        name="score_far",
    )(where, queries, pos, *embs, *packs, *near_packs, state)


def merge_kernel(parts_ref, loss_ref, ids_ref):
    part = parts_ref[:, 0:PART_POS, :]
    highest = jnp.max(part, axis=0)
    summed = jnp.sum(jnp.exp2(part - highest[None]), axis=0)
    hit = jnp.sum(parts_ref[:, PART_POS:PART_IDS, :], axis=0)
    loss_ref[...] = jnp.log(summed) + (highest - hit) * LN2
    for a in range(N_COLS // 8):
        found = jnp.sum(parts_ref[a * 8 : (a + 1) * 8, PART_IDS:PART_ROWS, :], axis=0).astype(I32)
        for r in range(N_ROWS):
            ids_ref[r * (N_COLS // 8) + a : r * (N_COLS // 8) + a + 1, :] = found[r : r + 1, :]


def merge(parts):
    vmem_spec = pl.BlockSpec(memory_space=pltpu.VMEM)
    return pl.pallas_call(
        merge_kernel,
        in_specs=[vmem_spec],
        out_specs=[vmem_spec, vmem_spec],
        out_shape=[
            jax.ShapeDtypeStruct((QDEV // LANES, LANES), F32),
            jax.ShapeDtypeStruct((N_DEV * CAP // LANES, LANES), I32),
        ],
        name="merge",
    )(parts)


SWAP = [(0, 1), (1, 0)]


def local(features, w_in, w_out, item_ids, item_counts, owners, queries, positives):
    where = jnp.stack([lax.axis_index(ROWS), lax.axis_index(COLS)]).astype(I32)
    emb, send, pack = tower(
        features,
        w_in,
        w_out,
        owners.reshape(BLOCKS, LANES),
        item_ids.reshape(BLOCKS, LANES),
        item_counts.reshape(BLOCKS, LANES),
    )
    emb_y = lax.ppermute(emb, "rows_0", SWAP)
    pack_y = lax.ppermute(pack, "rows_0", SWAP)
    emb_c = lax.ppermute(emb, "rows_1", SWAP)
    pack_c = lax.ppermute(pack, "rows_1", SWAP)
    pool_emb = lax.all_to_all(send, ROWS_COLS, split_axis=0, concat_axis=0, tiled=True)
    emb_yc = lax.ppermute(emb_y, "rows_1", SWAP)
    pack_yc = lax.ppermute(pack_y, "rows_1", SWAP)
    pos = positives.reshape(-1, LANES)
    state = score_near(where, queries, pos, (emb, emb_c), (pack, pack_c))
    parts = score_far(
        where, queries, pos, (emb_y, emb_yc), (pack_y, pack_yc), (pack, pack_c), state
    )
    parts = lax.all_to_all(parts, COLS, split_axis=0, concat_axis=0, tiled=True)
    loss, ids = merge(parts)
    return (pool_emb, ids.reshape(-1), loss.reshape(-1))


def solution(mesh):
    torus = Mesh(
        mesh.devices.reshape(2, 2, 2, 4, 4), ("rows_0", "rows_1", "cols_0", "cols_1", "cols_2")
    )
    placed = (
        P(ROWS_COLS, None),
        P(),
        P(),
        P(ROWS_COLS),
        P(ROWS_COLS),
        P(ROWS_COLS, None),
        P(ROWS, None),
        P(),
    )
    return jax.shard_map(
        local,
        mesh=torus,
        in_specs=placed,
        out_specs=(P(ROWS_COLS, None), P(ROWS_COLS), P(ROWS)),
        check_vma=False,
    )
```

```python
import math

import jax
import jax.numpy as jnp
from jax import lax
from jax.experimental import pallas as pl
from jax.experimental.pallas import tpu as pltpu
from jax.sharding import Mesh
from jax.sharding import PartitionSpec as P

ROWS = ("rows_0", "rows_1")
COLS = ("cols_0", "cols_1", "cols_2")
ROWS_COLS = ("rows_0", "rows_1", "cols_0", "cols_1", "cols_2")

F32 = jnp.float32
BF16 = jnp.bfloat16
I32 = jnp.int32

N_DEV = 128
N_ROWS = 4
N_COLS = 32
ITEMS = 1024
CAP = 16
EMB = 256
HID = 1024
F_IN = 2048
QDEV = 2048
LANES = 128
BLOCKS = ITEMS // LANES

LOG2E = math.log2(math.e)
LN2 = math.log(2.0)
SCALE2 = 4.0 / math.sqrt(EMB) * LOG2E
FLOOR = -1e30

EXT_SLOTS = ITEMS
EXT_A = EXT_SLOTS + N_DEV // 2
EXT_B = EXT_A + 16
EXT_C = EXT_B + 16
EXT_ROWS = EXT_C + 16

PART_POS = QDEV // LANES
PART_IDS = 2 * PART_POS
PART_ROWS = PART_IDS + 8

NT = (((1,), (1,)), ((), ()))

K_CHUNK = 512
K_STEPS = F_IN // K_CHUNK
ROW_BLOCK = 256


def tower_kernel(
    feat_hbm, w_in_hbm, w_out_hbm, owners_hbm, ids_hbm, counts_hbm,
    ext_ref, send_ref,
    feat, w_in, w_out, acc, owners_ref, ids_ref, counts_ref, slots,
    feat_sem, w_in_sem, w_out_sem, small_sem,
):
    small = [
        pltpu.make_async_copy(held, ref, small_sem.at[k])
        for k, (held, ref) in enumerate(
            ((owners_hbm, owners_ref), (ids_hbm, ids_ref), (counts_hbm, counts_ref))
        )
    ]
    for copy in small:
        copy.start()
    copies = []
    for k in range(K_STEPS):
        at = pl.ds(k * K_CHUNK, K_CHUNK)
        copies.append(
            (
                pltpu.make_async_copy(w_in_hbm.at[at], w_in.at[at], w_in_sem.at[k]),
                pltpu.make_async_copy(feat_hbm.at[:, at], feat.at[:, at], feat_sem.at[k]),
            )
        )
    w_out_copy = pltpu.make_async_copy(w_out_hbm, w_out, w_out_sem)
    for k in range(2):
        for copy in copies[k]:
            copy.start()

    for copy in small:
        copy.wait()

    owner_iota = lax.broadcasted_iota(I32, (N_DEV, LANES), 0)
    row_iota = lax.broadcasted_iota(I32, (LANES, LANES), 0)
    upper = (row_iota < lax.broadcasted_iota(I32, (LANES, LANES), 1)).astype(F32).astype(BF16)
    seen = jnp.zeros((N_DEV, 1), F32)
    by_slot = jnp.zeros((N_DEV, LANES), F32)
    for j in range(BLOCKS):
        owner = owners_ref[j : j + 1, :]
        onehot = (owner_iota == owner).astype(F32)
        onehot_b = onehot.astype(BF16)
        before = jnp.dot(onehot_b, upper, preferred_element_type=F32) + seen
        rank = jnp.sum(onehot * before, axis=0, keepdims=True).astype(I32)
        seen = seen + jnp.sum(onehot, axis=1, keepdims=True)
        slots[j : j + 1, :] = owner * CAP + rank
        value = ids_ref[j : j + 1, :] + 1
        piece = jnp.where(
            row_iota < CAP,
            value >> 12,
            jnp.where(row_iota < 2 * CAP, (value >> 6) & 63, value & 63),
        )
        here = (row_iota % CAP == rank) & (row_iota < 3 * CAP)
        chosen = jnp.where(here, piece, 0).astype(F32).astype(BF16)
        by_slot = by_slot + lax.dot_general(onehot_b, chosen, NT, preferred_element_type=F32)
    half = N_DEV // 2
    ext_ref[EXT_SLOTS:EXT_A, 0:LANES] = by_slot[0:half, :].astype(BF16)
    ext_ref[EXT_SLOTS:EXT_A, LANES:EMB] = by_slot[half:N_DEV, :].astype(BF16)
    ids = ids_ref[...]
    counts = counts_ref[...]
    none = jnp.zeros((BLOCKS, LANES), I32)
    for at, left, right in (
        (EXT_A, ids >> 12, (ids >> 6) & 63),
        (EXT_B, ids & 63, counts >> 8),
        (EXT_C, counts & 255, none),
    ):
        for lanes, piece in ((slice(0, LANES), left), (slice(LANES, EMB), right)):
            ext_ref[at : at + 16, lanes] = (
                jnp.concatenate([piece, none], axis=0).astype(F32).astype(BF16)
            )

    for k in range(K_STEPS):
        for copy in copies[k]:
            copy.wait()
        if k + 2 < K_STEPS:
            for copy in copies[k + 2]:
                copy.start()
        if k + 2 == K_STEPS:
            w_out_copy.start()
        last = k == K_STEPS - 1
        if last:
            w_out_copy.wait()
        at = slice(k * K_CHUNK, (k + 1) * K_CHUNK)
        for b in range(ITEMS // ROW_BLOCK):
            rows = slice(b * ROW_BLOCK, (b + 1) * ROW_BLOCK)
            part = jnp.dot(feat[rows, at], w_in[at, :], preferred_element_type=F32)
            if k > 0:
                part = acc[rows, :] + part
            if not last:
                acc[rows, :] = part
            else:
                hidden = jnp.maximum(part, 0.0).astype(BF16)
                ext_ref[rows, :] = jnp.dot(
                    hidden, w_out[...], preferred_element_type=F32
                ).astype(BF16)

    chunk = 512
    slot_row = jnp.concatenate([slots[j : j + 1, :] for j in range(BLOCKS)], axis=1)
    for c in range(N_DEV * CAP // chunk):
        place = lax.broadcasted_iota(I32, (chunk, ITEMS), 0) + c * chunk
        chosen = (place == slot_row).astype(F32).astype(BF16)
        send_ref[c * chunk : (c + 1) * chunk, :] = jnp.dot(
            chosen, ext_ref[0:ITEMS, :], preferred_element_type=F32
        ).astype(BF16)


VMEM_SPEC = pl.BlockSpec(memory_space=pltpu.VMEM)
ANY_SPEC = pl.BlockSpec(memory_space=pl.ANY)
SMEM_SPEC = pl.BlockSpec(memory_space=pltpu.SMEM)


def near_core(value):
    return pltpu.with_memory_space_constraint(value, pltpu.VMEM)


def in_hbm(value):
    return pltpu.with_memory_space_constraint(value, pltpu.HBM)


def tower(features, w_in, w_out, owners, ids, counts):
    return pl.pallas_call(
        tower_kernel,
        in_specs=[ANY_SPEC] * 6,
        out_specs=[VMEM_SPEC, VMEM_SPEC],
        out_shape=[
            pltpu.VMEM((EXT_ROWS, EMB), BF16),
            pltpu.VMEM((N_DEV * CAP, EMB), BF16),
        ],
        scratch_shapes=[
            pltpu.VMEM((ITEMS, F_IN), BF16),
            pltpu.VMEM((F_IN, HID), BF16),
            pltpu.VMEM((HID, EMB), BF16),
            pltpu.VMEM((ITEMS, HID), F32),
            pltpu.VMEM((BLOCKS, LANES), I32),
            pltpu.VMEM((BLOCKS, LANES), I32),
            pltpu.VMEM((BLOCKS, LANES), I32),
            pltpu.VMEM((BLOCKS, LANES), I32),
            pltpu.SemaphoreType.DMA((K_STEPS,)),
            pltpu.SemaphoreType.DMA((K_STEPS,)),
            pltpu.SemaphoreType.DMA,
            pltpu.SemaphoreType.DMA((3,)),
        ],
        cost_estimate=pl.CostEstimate(
            flops=2 * ITEMS * F_IN * HID + 2 * ITEMS * HID * EMB,
            bytes_accessed=2 * (ITEMS * F_IN + F_IN * HID),
            transcendentals=0,
        ),
        compiler_params=pltpu.CompilerParams(vmem_limit_bytes=28 << 20),
        name="tower",
    )(*[in_hbm(a) for a in (features, w_in, w_out, owners, ids, counts)])


Q_TILE = 256
Q_PARTS = Q_TILE // LANES
Q_STEPS = QDEV // Q_TILE
I_TILE = 512
GROUPS = I_TILE // 8


def unpack_columns(exts, col_ids, col_logq):
    fill = jnp.zeros((LANES - BLOCKS, LANES), F32)
    for n, ext in enumerate(exts):
        a, b, c = [ext[at : at + 16, :].astype(F32) for at in (EXT_A, EXT_B, EXT_C)]
        a, b, c = a[0:BLOCKS], b[0:BLOCKS], c[0:BLOCKS]
        ids = a[:, 0:LANES] * 4096.0 + a[:, LANES:EMB] * 64.0 + b[:, 0:LANES]
        logq = jnp.log(b[:, LANES:EMB] * 256.0 + c[:, 0:LANES] + 1.0) * LOG2E
        for value, col in ((ids, col_ids), (logq, col_logq)):
            turned = jnp.concatenate([value, fill], axis=0).T
            for j in range(BLOCKS):
                at = n * ITEMS + j * LANES
                col[at : at + LANES, :] = jnp.broadcast_to(turned[:, j : j + 1], (LANES, LANES))


def score_blocks(q_ref, pos_ref, exts, col_ids, col_logq, before, after):
    unpack_columns(exts, col_ids, col_logq)

    def tile_inputs(t):
        q_rows = q_ref[pl.ds(pl.multiple_of(t * Q_TILE, Q_TILE), Q_TILE), :]
        pos_row = jnp.concatenate(
            [pos_ref[pl.ds(t * Q_PARTS + u, 1), :].astype(F32) for u in range(Q_PARTS)], axis=1
        )
        return q_rows, jnp.broadcast_to(pos_row, (8, Q_TILE))

    def raw_scores(q_rows, n, c):
        return lax.dot_general(
            exts[n][c * I_TILE : (c + 1) * I_TILE, :], q_rows, NT, preferred_element_type=F32
        )

    def wide(col, at):
        return jnp.concatenate([col[at : at + 8, :]] * Q_PARTS, axis=1)

    chunks = [(n, c) for n in range(len(exts)) for c in range(ITEMS // I_TILE)]

    def fast_tile(t, worst):
        q_rows, pos8 = tile_inputs(t)
        if before is None:
            raw = raw_scores(q_rows, 0, 0)
            tops = [jnp.full((8, Q_TILE), FLOOR, F32)] * 4
            for g in range(GROUPS):
                logit = raw[g * 8 : g * 8 + 8, :] * SCALE2 - wide(col_logq, g * 8)
                tops[g % 4] = jnp.maximum(tops[g % 4], logit)
            top = jnp.maximum(jnp.maximum(tops[0], tops[1]), jnp.maximum(tops[2], tops[3]))
            shift = jnp.broadcast_to(jnp.max(top, axis=0, keepdims=True), (8, Q_TILE))
            total = jnp.zeros((8, Q_TILE), F32)
            hit = jnp.full((8, Q_TILE), FLOOR, F32)
        else:
            shift, total, hit = [before[k, t] for k in range(3)]
        totals = [total, jnp.zeros((8, Q_TILE), F32)]
        hits = [hit, jnp.full((8, Q_TILE), FLOOR, F32)]
        for n, c in chunks:
            raw = raw_scores(q_rows, n, c)
            for g in range(GROUPS):
                at = n * ITEMS + c * I_TILE + g * 8
                logit = raw[g * 8 : g * 8 + 8, :] * SCALE2 - wide(col_logq, at) - shift
                totals[g % 2] = totals[g % 2] + jnp.exp2(logit)
                hits[g % 2] = jnp.where(wide(col_ids, at) == pos8, logit, hits[g % 2])
        total = totals[0] + totals[1]
        after[0, t] = shift
        after[1, t] = total
        after[2, t] = jnp.maximum(hits[0], hits[1])
        return jnp.maximum(worst, total)

    worst = lax.fori_loop(0, Q_STEPS, fast_tile, jnp.zeros((8, Q_TILE), F32))

    @pl.when(jnp.logical_not(jnp.max(worst) < 1e37))
    def _():
        def safe_tile(t, _):
            q_rows, pos8 = tile_inputs(t)
            if before is None:
                top = jnp.full((8, Q_TILE), FLOOR, F32)
                total = jnp.zeros((8, Q_TILE), F32)
                hit = jnp.full((8, Q_TILE), FLOOR, F32)
            else:
                top, total, hit = [before[k, t] for k in range(3)]
            found = hit > FLOOR / 2
            positive = jnp.where(found, hit + top, 0.0)
            for n, c in chunks:
                raw = raw_scores(q_rows, n, c)
                at = slice(n * ITEMS + c * I_TILE, n * ITEMS + (c + 1) * I_TILE)
                logit = raw * SCALE2 - jnp.concatenate([col_logq[at, :]] * Q_PARTS, axis=1)
                match = jnp.concatenate([col_ids[at, :]] * Q_PARTS, axis=1) == pos8[0:1]
                grouped = logit.reshape(GROUPS, 8, Q_TILE)
                new_top = jnp.maximum(top, jnp.max(grouped, axis=0))
                total = total * jnp.exp2(top - new_top) + jnp.sum(
                    jnp.exp2(grouped - new_top[None]), axis=0
                )
                positive = positive + jnp.sum(
                    jnp.where(match, logit, 0.0).reshape(GROUPS, 8, Q_TILE), axis=0
                )
                found = found | (
                    jnp.max(match.astype(F32).reshape(GROUPS, 8, Q_TILE), axis=0) > 0.0
                )
                top = new_top
            after[0, t] = top
            after[1, t] = total
            after[2, t] = jnp.where(found, positive - top, FLOOR)
            return 0

        lax.fori_loop(0, Q_STEPS, safe_tile, 0)


def own_positives(where_ref, pos_all):
    return pos_all.at[pl.ds(where_ref[0] * (QDEV // LANES), QDEV // LANES)]


def first_kernel(where_ref, q_ref, pos_all, ext0, ext1, state_ref, col_ids, col_logq):
    pos_ref = own_positives(where_ref, pos_all)
    score_blocks(q_ref, pos_ref, (ext0, ext1), col_ids, col_logq, None, state_ref)


def next_kernel(where_ref, q_ref, pos_all, ext, before_ref, state_ref, col_ids, col_logq):
    pos_ref = own_positives(where_ref, pos_all)
    score_blocks(q_ref, pos_ref, (ext,), col_ids, col_logq, before_ref, state_ref)


def last_kernel(
    where_ref, q_ref, pos_all, ext, before_ref, own, sibling, across,
    out_ref, state, parts, col_ids, col_logq,
):
    row = where_ref[0]
    col = where_ref[1]
    pos_ref = own_positives(where_ref, pos_all)
    score_blocks(q_ref, pos_ref, (ext,), col_ids, col_logq, before_ref, state)

    for t in range(Q_STEPS):
        top, total, hit = [state[k, t] for k in range(3)]
        highest = jnp.max(top, axis=0, keepdims=True)
        summed = jnp.sum(total * jnp.exp2(top - highest), axis=0, keepdims=True)
        positive = jnp.sum(jnp.where(hit > FLOOR / 2, hit + top, 0.0), axis=0, keepdims=True)
        both = (highest + jnp.log(summed) * LOG2E, positive)
        for k in range(2):
            for u in range(Q_PARTS):
                at = k * PART_POS + t * Q_PARTS + u
                parts[at : at + 1, :] = both[k][:, u * LANES : (u + 1) * LANES]
    out_ref[:, 0:PART_IDS, :] = jnp.broadcast_to(parts[...][None], (N_COLS, PART_IDS, LANES))

    lane = lax.broadcasted_iota(I32, (N_COLS, LANES), 1)
    place = lax.broadcasted_iota(I32, (N_COLS, 8, LANES), 1)
    slots = pl.ds(EXT_SLOTS + (row % 2) * N_COLS, N_COLS)
    found = jnp.zeros((N_COLS, 8, LANES), F32)
    for source, held in ((row, own), (row ^ 1, sibling), (row ^ 2, across), (row ^ 3, ext)):
        piece = jnp.where(row >= 2, held[slots, LANES:EMB].astype(F32), held[slots, 0:LANES].astype(F32))
        value = (
            piece * 4096.0
            + pltpu.roll(piece, LANES - CAP, 1) * 64.0
            + pltpu.roll(piece, LANES - 2 * CAP, 1)
            - 1.0
        )
        value = pltpu.roll(jnp.where(lane < CAP, value, 0.0), (col % 8) * CAP, 1)
        found = jnp.where(
            place == source, jnp.broadcast_to(value[:, None, :], (N_COLS, 8, LANES)), found
        )
    out_ref[:, PART_IDS:PART_ROWS, :] = found


STATE = ((3, Q_STEPS, 8, Q_TILE), F32)


def scored(kernel, n_blocks, out_shape, scratch, args, name):
    columns = [pltpu.VMEM((n_blocks * ITEMS, LANES), F32)] * 2
    return pl.pallas_call(
        kernel,
        in_specs=[SMEM_SPEC] + [VMEM_SPEC] * (len(args) - 1),
        out_specs=VMEM_SPEC,
        out_shape=pltpu.VMEM(*out_shape),
        scratch_shapes=scratch + columns,
        cost_estimate=pl.CostEstimate(
            flops=2 * QDEV * n_blocks * ITEMS * EMB,
            bytes_accessed=2 * (QDEV * EMB + n_blocks * ITEMS * EMB),
            transcendentals=QDEV * n_blocks * ITEMS,
        ),
        compiler_params=pltpu.CompilerParams(vmem_limit_bytes=20 << 20),
        name=name,
    )(args[0], *[near_core(a) for a in args[1:]])


def merge_kernel(parts_ref, pool_in, loss_ref, ids_ref, pool_out, sem):
    copy = pltpu.make_async_copy(pool_in, pool_out, sem)
    copy.start()
    part = parts_ref[:, 0:PART_POS, :]
    highest = jnp.max(part, axis=0)
    summed = jnp.sum(jnp.exp2(part - highest[None]), axis=0)
    hit = jnp.sum(parts_ref[:, PART_POS:PART_IDS, :], axis=0)
    loss_ref[...] = jnp.log(summed) + (highest - hit) * LN2
    for a in range(N_COLS // 8):
        found = jnp.sum(parts_ref[a * 8 : (a + 1) * 8, PART_IDS:PART_ROWS, :], axis=0).astype(I32)
        for r in range(N_ROWS):
            ids_ref[r * (N_COLS // 8) + a : r * (N_COLS // 8) + a + 1, :] = found[r : r + 1, :]
    copy.wait()


def merge(parts, pool):
    return pl.pallas_call(
        merge_kernel,
        in_specs=[VMEM_SPEC, VMEM_SPEC],
        out_specs=[VMEM_SPEC, VMEM_SPEC, ANY_SPEC],
        out_shape=[
            jax.ShapeDtypeStruct((QDEV // LANES, LANES), F32),
            jax.ShapeDtypeStruct((N_DEV * CAP // LANES, LANES), I32),
            pltpu.HBM(pool.shape, pool.dtype),
        ],
        scratch_shapes=[pltpu.SemaphoreType.DMA],
        compiler_params=pltpu.CompilerParams(vmem_limit_bytes=8 << 20),
        name="merge",
    )(near_core(parts), near_core(pool))


SWAP = [(0, 1), (1, 0)]


def local(features, w_in, w_out, item_ids, item_counts, owners, queries, positives):
    where = jnp.stack([lax.axis_index(ROWS), lax.axis_index(COLS)]).astype(I32)
    pos = positives.reshape(-1, LANES)
    own, send = tower(
        features,
        w_in,
        w_out,
        owners.reshape(BLOCKS, LANES),
        item_ids.reshape(BLOCKS, LANES),
        item_counts.reshape(BLOCKS, LANES),
    )
    across = lax.ppermute(own, "rows_0", SWAP)
    sibling = lax.ppermute(own, "rows_1", SWAP)
    pool_emb = lax.all_to_all(send, ROWS_COLS, split_axis=0, concat_axis=0, tiled=True)
    state = scored(first_kernel, 2, STATE, [], (where, queries, pos, own, sibling), "score_first")
    across, state = lax.optimization_barrier((across, state))
    far = lax.ppermute(across, "rows_1", SWAP)
    state = scored(next_kernel, 1, STATE, [], (where, queries, pos, across, state), "score_next")
    parts = scored(
        last_kernel,
        1,
        ((N_COLS, PART_ROWS, LANES), F32),
        [pltpu.VMEM(*STATE), pltpu.VMEM((PART_IDS, LANES), F32)],
        (where, queries, pos, far, state, own, sibling, across),
        "score_last",
    )
    parts = lax.all_to_all(parts, COLS, split_axis=0, concat_axis=0, tiled=True)
    loss, ids, pool_emb = merge(parts, pool_emb)
    return (pool_emb, ids.reshape(-1), loss.reshape(-1))


def solution(mesh):
    torus = Mesh(
        mesh.devices.reshape(2, 2, 2, 4, 4), ("rows_0", "rows_1", "cols_0", "cols_1", "cols_2")
    )
    placed = (
        P(ROWS_COLS, None),
        P(),
        P(),
        P(ROWS_COLS),
        P(ROWS_COLS),
        P(ROWS_COLS, None),
        P(ROWS, None),
        P(),
    )
    return jax.shard_map(
        local,
        mesh=torus,
        in_specs=placed,
        out_specs=(P(ROWS_COLS, None), P(ROWS_COLS), P(ROWS)),
        check_vma=False,
    )
```

```python
import math

import jax
import jax.numpy as jnp
from jax import lax
from jax.experimental import pallas as pl
from jax.experimental.pallas import tpu as pltpu
from jax.sharding import Mesh
from jax.sharding import PartitionSpec as P

ROWS = ("rows_0", "rows_1")
COLS = ("cols_0", "cols_1", "cols_2")
ROWS_COLS = ("rows_0", "rows_1", "cols_0", "cols_1", "cols_2")

F32 = jnp.float32
BF16 = jnp.bfloat16
I32 = jnp.int32

N_DEV = 128
N_ROWS = 4
N_COLS = 32
ITEMS = 1024
CAP = 16
EMB = 256
HID = 1024
F_IN = 2048
QDEV = 2048
LANES = 128
BLOCKS = ITEMS // LANES

LOG2E = math.log2(math.e)
LN2 = math.log(2.0)
SCALE2 = 4.0 / math.sqrt(EMB) * LOG2E
FLOOR = -1e30

EXT_SLOTS = ITEMS
EXT_A = EXT_SLOTS + N_DEV // 2
EXT_B = EXT_A + 16
EXT_C = EXT_B + 16
EXT_ROWS = EXT_C + 16

PART_POS = QDEV // LANES
PART_IDS = 2 * PART_POS
PART_ROWS = PART_IDS + 8

NT = (((1,), (1,)), ((), ()))

K_CHUNK = 512
K_STEPS = F_IN // K_CHUNK
ROW_BLOCK = 256


def tower_kernel(
    feat_hbm, w_in_hbm, w_out_hbm, owners_hbm, ids_hbm, counts_hbm,
    ext_ref, send_ref,
    feat, w_in, w_out, acc, owners_ref, ids_ref, counts_ref, slots,
    feat_sem, w_in_sem, w_out_sem, small_sem,
):
    small = [
        pltpu.make_async_copy(held, ref, small_sem.at[k])
        for k, (held, ref) in enumerate(
            ((owners_hbm, owners_ref), (ids_hbm, ids_ref), (counts_hbm, counts_ref))
        )
    ]
    for copy in small:
        copy.start()
    copies = []
    for k in range(K_STEPS):
        at = pl.ds(k * K_CHUNK, K_CHUNK)
        copies.append(
            (
                pltpu.make_async_copy(w_in_hbm.at[at], w_in.at[at], w_in_sem.at[k]),
                pltpu.make_async_copy(feat_hbm.at[:, at], feat.at[:, at], feat_sem.at[k]),
            )
        )
    w_out_copy = pltpu.make_async_copy(w_out_hbm, w_out, w_out_sem)
    for k in range(2):
        for copy in copies[k]:
            copy.start()

    for copy in small:
        copy.wait()

    owner_iota = lax.broadcasted_iota(I32, (N_DEV, LANES), 0)
    row_iota = lax.broadcasted_iota(I32, (LANES, LANES), 0)
    upper = (row_iota < lax.broadcasted_iota(I32, (LANES, LANES), 1)).astype(F32).astype(BF16)
    seen = jnp.zeros((N_DEV, 1), F32)
    by_slot = jnp.zeros((N_DEV, LANES), F32)
    for j in range(BLOCKS):
        owner = owners_ref[j : j + 1, :]
        onehot = (owner_iota == owner).astype(F32)
        onehot_b = onehot.astype(BF16)
        before = jnp.dot(onehot_b, upper, preferred_element_type=F32) + seen
        rank = jnp.sum(onehot * before, axis=0, keepdims=True).astype(I32)
        seen = seen + jnp.sum(onehot, axis=1, keepdims=True)
        slots[j : j + 1, :] = owner * CAP + rank
        value = ids_ref[j : j + 1, :] + 1
        piece = jnp.where(
            row_iota < CAP,
            value >> 12,
            jnp.where(row_iota < 2 * CAP, (value >> 6) & 63, value & 63),
        )
        here = (row_iota % CAP == rank) & (row_iota < 3 * CAP)
        chosen = jnp.where(here, piece, 0).astype(F32).astype(BF16)
        by_slot = by_slot + lax.dot_general(onehot_b, chosen, NT, preferred_element_type=F32)
    half = N_DEV // 2
    ext_ref[EXT_SLOTS:EXT_A, 0:LANES] = by_slot[0:half, :].astype(BF16)
    ext_ref[EXT_SLOTS:EXT_A, LANES:EMB] = by_slot[half:N_DEV, :].astype(BF16)
    ids = ids_ref[...]
    counts = counts_ref[...]
    none = jnp.zeros((BLOCKS, LANES), I32)
    for at, left, right in (
        (EXT_A, ids >> 12, (ids >> 6) & 63),
        (EXT_B, ids & 63, counts >> 8),
        (EXT_C, counts & 255, none),
    ):
        for lanes, piece in ((slice(0, LANES), left), (slice(LANES, EMB), right)):
            ext_ref[at : at + 16, lanes] = (
                jnp.concatenate([piece, none], axis=0).astype(F32).astype(BF16)
            )

    for k in range(K_STEPS):
        for copy in copies[k]:
            copy.wait()
        if k + 2 < K_STEPS:
            for copy in copies[k + 2]:
                copy.start()
        if k + 2 == K_STEPS:
            w_out_copy.start()
        last = k == K_STEPS - 1
        if last:
            w_out_copy.wait()
        at = slice(k * K_CHUNK, (k + 1) * K_CHUNK)
        for b in range(ITEMS // ROW_BLOCK):
            rows = slice(b * ROW_BLOCK, (b + 1) * ROW_BLOCK)
            part = jnp.dot(feat[rows, at], w_in[at, :], preferred_element_type=F32)
            if k > 0:
                part = acc[rows, :] + part
            if not last:
                acc[rows, :] = part
            else:
                hidden = jnp.maximum(part, 0.0).astype(BF16)
                ext_ref[rows, :] = jnp.dot(
                    hidden, w_out[...], preferred_element_type=F32
                ).astype(BF16)

    chunk = 512
    slot_row = jnp.concatenate([slots[j : j + 1, :] for j in range(BLOCKS)], axis=1)
    for c in range(N_DEV * CAP // chunk):
        place = lax.broadcasted_iota(I32, (chunk, ITEMS), 0) + c * chunk
        chosen = (place == slot_row).astype(F32).astype(BF16)
        send_ref[c * chunk : (c + 1) * chunk, :] = jnp.dot(
            chosen, ext_ref[0:ITEMS, :], preferred_element_type=F32
        ).astype(BF16)


VMEM_SPEC = pl.BlockSpec(memory_space=pltpu.VMEM)
ANY_SPEC = pl.BlockSpec(memory_space=pl.ANY)


def near_core(value):
    return pltpu.with_memory_space_constraint(value, pltpu.VMEM)


def in_hbm(value):
    return pltpu.with_memory_space_constraint(value, pltpu.HBM)


def tower(features, w_in, w_out, owners, ids, counts):
    return pl.pallas_call(
        tower_kernel,
        in_specs=[ANY_SPEC] * 6,
        out_specs=[VMEM_SPEC, VMEM_SPEC],
        out_shape=[
            pltpu.VMEM((EXT_ROWS, EMB), BF16),
            pltpu.VMEM((N_DEV * CAP, EMB), BF16),
        ],
        scratch_shapes=[
            pltpu.VMEM((ITEMS, F_IN), BF16),
            pltpu.VMEM((F_IN, HID), BF16),
            pltpu.VMEM((HID, EMB), BF16),
            pltpu.VMEM((ITEMS, HID), F32),
            pltpu.VMEM((BLOCKS, LANES), I32),
            pltpu.VMEM((BLOCKS, LANES), I32),
            pltpu.VMEM((BLOCKS, LANES), I32),
            pltpu.VMEM((BLOCKS, LANES), I32),
            pltpu.SemaphoreType.DMA((K_STEPS,)),
            pltpu.SemaphoreType.DMA((K_STEPS,)),
            pltpu.SemaphoreType.DMA,
            pltpu.SemaphoreType.DMA((3,)),
        ],
        cost_estimate=pl.CostEstimate(
            flops=2 * ITEMS * F_IN * HID + 2 * ITEMS * HID * EMB,
            bytes_accessed=2 * (ITEMS * F_IN + F_IN * HID),
            transcendentals=0,
        ),
        compiler_params=pltpu.CompilerParams(vmem_limit_bytes=28 << 20),
        name="tower",
    )(*[in_hbm(a) for a in (features, w_in, w_out, owners, ids, counts)])


Q_TILE = 256
Q_PARTS = Q_TILE // LANES
Q_STEPS = QDEV // Q_TILE
I_TILE = 512
GROUPS = I_TILE // 8
SAMPLE = 16


def row_index():
    return lax.axis_index("rows_0") * 2 + lax.axis_index("rows_1")


def unpack_columns(exts, col_ids, col_logq):
    fill = jnp.zeros((LANES - BLOCKS, LANES), F32)
    for n, ext in enumerate(exts):
        a, b, c = [ext[at : at + 16, :].astype(F32) for at in (EXT_A, EXT_B, EXT_C)]
        a, b, c = a[0:BLOCKS], b[0:BLOCKS], c[0:BLOCKS]
        ids = a[:, 0:LANES] * 4096.0 + a[:, LANES:EMB] * 64.0 + b[:, 0:LANES]
        logq = jnp.log(b[:, LANES:EMB] * 256.0 + c[:, 0:LANES] + 1.0) * LOG2E
        for value, col in ((ids, col_ids), (logq, col_logq)):
            turned = jnp.concatenate([value, fill], axis=0).T
            for j in range(BLOCKS):
                at = n * ITEMS + j * LANES
                col[at : at + LANES, :] = jnp.broadcast_to(turned[:, j : j + 1], (LANES, LANES))


def score_tiles(q_ref, pos_all, row, tiles, exts, col_ids, col_logq, out_ref):
    first, count = tiles
    out_rows = count * Q_PARTS

    def tile_inputs(t):
        q_rows = q_ref[pl.ds(pl.multiple_of(t * Q_TILE, Q_TILE), Q_TILE), :]
        at = row * (QDEV // LANES) + t * Q_PARTS
        pos_row = jnp.concatenate(
            [pos_all[pl.ds(at + u, 1), :].astype(F32) for u in range(Q_PARTS)], axis=1
        )
        return q_rows, jnp.broadcast_to(pos_row, (8, Q_TILE))

    def raw_scores(q_rows, n, c):
        return lax.dot_general(
            exts[n][c * I_TILE : (c + 1) * I_TILE, :], q_rows, NT, preferred_element_type=F32
        )

    def wide(col, at):
        return jnp.concatenate([col[at : at + 8, :]] * Q_PARTS, axis=1)

    def finish(t, top, total, positive):
        highest = jnp.max(top, axis=0, keepdims=True)
        summed = jnp.sum(total * jnp.exp2(top - highest), axis=0, keepdims=True)
        both = (highest + jnp.log(summed) * LOG2E, jnp.sum(positive, axis=0, keepdims=True))
        for k in range(2):
            for u in range(Q_PARTS):
                at = k * out_rows + (t - first) * Q_PARTS + u
                out_ref[pl.ds(at, 1), :] = both[k][:, u * LANES : (u + 1) * LANES]

    chunks = [(n, c) for n in range(len(exts)) for c in range(ITEMS // I_TILE)]

    def fast_tile(t, worst):
        q_rows, pos8 = tile_inputs(t)
        shift = None
        totals = [jnp.zeros((8, Q_TILE), F32)] * 2
        hits = [jnp.full((8, Q_TILE), FLOOR, F32)] * 2
        for n, c in chunks:
            raw = raw_scores(q_rows, n, c)
            if shift is None:
                tops = [jnp.full((8, Q_TILE), FLOOR, F32)] * 2
                for g in range(SAMPLE):
                    logit = raw[g * 8 : g * 8 + 8, :] * SCALE2 - wide(col_logq, g * 8)
                    tops[g % 2] = jnp.maximum(tops[g % 2], logit)
                top = jnp.maximum(tops[0], tops[1])
                shift = jnp.broadcast_to(jnp.max(top, axis=0, keepdims=True), (8, Q_TILE))
            for g in range(GROUPS):
                at = n * ITEMS + c * I_TILE + g * 8
                logit = raw[g * 8 : g * 8 + 8, :] * SCALE2 - wide(col_logq, at) - shift
                totals[g % 2] = totals[g % 2] + jnp.exp2(logit)
                hits[g % 2] = jnp.where(wide(col_ids, at) == pos8, logit, hits[g % 2])
        total = totals[0] + totals[1]
        hit = jnp.maximum(hits[0], hits[1])
        finish(t, shift, total, jnp.where(hit > FLOOR / 2, hit + shift, 0.0))
        return jnp.maximum(worst, total)

    worst = lax.fori_loop(first, first + count, fast_tile, jnp.zeros((8, Q_TILE), F32))

    @pl.when(jnp.logical_not(jnp.max(worst) < 1e37))
    def _():
        def safe_tile(t, _):
            q_rows, pos8 = tile_inputs(t)
            top = jnp.full((8, Q_TILE), FLOOR, F32)
            total = jnp.zeros((8, Q_TILE), F32)
            positive = jnp.zeros((8, Q_TILE), F32)
            for n, c in chunks:
                raw = raw_scores(q_rows, n, c)
                at = slice(n * ITEMS + c * I_TILE, n * ITEMS + (c + 1) * I_TILE)
                logit = raw * SCALE2 - jnp.concatenate([col_logq[at, :]] * Q_PARTS, axis=1)
                match = jnp.concatenate([col_ids[at, :]] * Q_PARTS, axis=1) == pos8[0:1]
                grouped = logit.reshape(GROUPS, 8, Q_TILE)
                new_top = jnp.maximum(top, jnp.max(grouped, axis=0))
                total = total * jnp.exp2(top - new_top) + jnp.sum(
                    jnp.exp2(grouped - new_top[None]), axis=0
                )
                positive = positive + jnp.sum(
                    jnp.where(match, logit, 0.0).reshape(GROUPS, 8, Q_TILE), axis=0
                )
                top = new_top
            finish(t, top, total, positive)
            return 0

        lax.fori_loop(first, first + count, safe_tile, 0)


def slot_ids(held, row):
    shift = (lax.axis_index("cols_1") * 4 + lax.axis_index("cols_2")) % 8 * CAP
    lane = lax.broadcasted_iota(I32, (N_COLS, LANES), 1)
    slots = pl.ds(EXT_SLOTS + (row % 2) * N_COLS, N_COLS)
    piece = jnp.where(
        row >= 2, held[slots, LANES:EMB].astype(F32), held[slots, 0:LANES].astype(F32)
    )
    value = (
        piece * 4096.0
        + pltpu.roll(piece, LANES - CAP, 1) * 64.0
        + pltpu.roll(piece, LANES - 2 * CAP, 1)
        - 1.0
    )
    return pltpu.roll(jnp.where(lane < CAP, value, 0.0), shift, 1)


def score_and_list(q_ref, pos_all, exts, out_ref, col_ids, col_logq):
    row = row_index()
    unpack_columns(exts, col_ids, col_logq)
    for n, ext in enumerate(exts):
        out_ref[PART_IDS + n * N_COLS : PART_IDS + (n + 1) * N_COLS, :] = slot_ids(ext, row)
    score_tiles(q_ref, pos_all, row, (0, Q_STEPS), exts, col_ids, col_logq, out_ref)


def first_kernel(q_ref, pos_all, own, out_ref, col_ids, col_logq):
    score_and_list(q_ref, pos_all, (own,), out_ref, col_ids, col_logq)


def next_kernel(q_ref, pos_all, sibling, across, out_ref, col_ids, col_logq):
    score_and_list(q_ref, pos_all, (sibling, across), out_ref, col_ids, col_logq)


def last_kernel(q_ref, pos_all, far, first, middle, out_ref, last, col_ids, col_logq):
    score_and_list(q_ref, pos_all, (far,), last, col_ids, col_logq)
    held = (first, middle, last)
    sums = [ref[0:PART_POS, :] for ref in held]
    highest = jnp.maximum(jnp.maximum(sums[0], sums[1]), sums[2])
    total = sum(jnp.exp2(value - highest) for value in sums)
    positive = sum(ref[PART_POS:PART_IDS, :] for ref in held)
    parts = jnp.concatenate([highest + jnp.log(total) * LOG2E, positive], axis=0)
    out_ref[:, 0:PART_IDS, :] = jnp.broadcast_to(parts[None], (N_COLS, PART_IDS, LANES))

    row = row_index()
    place = lax.broadcasted_iota(I32, (N_COLS, 8, LANES), 1)
    found = jnp.zeros((N_COLS, 8, LANES), F32)
    for source, (ref, n) in enumerate(((first, 0), (middle, 0), (middle, 1), (last, 0))):
        ids = ref[PART_IDS + n * N_COLS : PART_IDS + (n + 1) * N_COLS, :]
        found = jnp.where(
            place == (row ^ source), jnp.broadcast_to(ids[:, None, :], (N_COLS, 8, LANES)), found
        )
    out_ref[:, PART_IDS:PART_ROWS, :] = found


def scored(kernel, n_blocks, out_shape, scratch, args, name):
    columns = [pltpu.VMEM((n_blocks * ITEMS, LANES), F32)] * 2
    return pl.pallas_call(
        kernel,
        in_specs=[VMEM_SPEC] * len(args),
        out_specs=VMEM_SPEC,
        out_shape=pltpu.VMEM(out_shape, F32),
        scratch_shapes=scratch + columns,
        cost_estimate=pl.CostEstimate(
            flops=2 * QDEV * n_blocks * ITEMS * EMB,
            bytes_accessed=2 * n_blocks * ITEMS * EMB,
            transcendentals=QDEV * n_blocks * ITEMS,
        ),
        compiler_params=pltpu.CompilerParams(vmem_limit_bytes=20 << 20),
        name=name,
    )(*[near_core(a) for a in args])


def merge_kernel(parts_ref, pool_in, loss_ref, ids_ref, pool_out, sem):
    copy = pltpu.make_async_copy(pool_in, pool_out, sem)
    copy.start()
    part = parts_ref[:, 0:PART_POS, :]
    highest = jnp.max(part, axis=0)
    summed = jnp.sum(jnp.exp2(part - highest[None]), axis=0)
    hit = jnp.sum(parts_ref[:, PART_POS:PART_IDS, :], axis=0)
    loss_ref[...] = jnp.log(summed) + (highest - hit) * LN2
    for a in range(N_COLS // 8):
        found = jnp.sum(parts_ref[a * 8 : (a + 1) * 8, PART_IDS:PART_ROWS, :], axis=0).astype(I32)
        for r in range(N_ROWS):
            ids_ref[r * (N_COLS // 8) + a : r * (N_COLS // 8) + a + 1, :] = found[r : r + 1, :]
    copy.wait()


def merge(parts, pool):
    return pl.pallas_call(
        merge_kernel,
        in_specs=[VMEM_SPEC, VMEM_SPEC],
        out_specs=[VMEM_SPEC, VMEM_SPEC, ANY_SPEC],
        out_shape=[
            jax.ShapeDtypeStruct((QDEV // LANES, LANES), F32),
            jax.ShapeDtypeStruct((N_DEV * CAP // LANES, LANES), I32),
            pltpu.HBM(pool.shape, pool.dtype),
        ],
        scratch_shapes=[pltpu.SemaphoreType.DMA],
        compiler_params=pltpu.CompilerParams(vmem_limit_bytes=8 << 20),
        name="merge",
    )(near_core(parts), near_core(pool))


SWAP = [(0, 1), (1, 0)]


def local(features, w_in, w_out, item_ids, item_counts, owners, queries, positives):
    pos = positives.reshape(-1, LANES)
    own, send = tower(
        features,
        w_in,
        w_out,
        owners.reshape(BLOCKS, LANES),
        item_ids.reshape(BLOCKS, LANES),
        item_counts.reshape(BLOCKS, LANES),
    )
    across = lax.ppermute(own, "rows_0", SWAP)
    sibling = lax.ppermute(own, "rows_1", SWAP)
    one = (PART_IDS + N_COLS, LANES)
    two = (PART_IDS + 2 * N_COLS, LANES)
    first = scored(first_kernel, 1, one, [], (queries, pos, own), "score_first")
    send, _ = lax.optimization_barrier((send, first))
    pool_emb = lax.all_to_all(send, ROWS_COLS, split_axis=0, concat_axis=0, tiled=True)
    far = lax.ppermute(across, "rows_1", SWAP)
    middle = scored(next_kernel, 2, two, [], (queries, pos, sibling, across), "score_next")
    parts = scored(
        last_kernel,
        1,
        (N_COLS, PART_ROWS, LANES),
        [pltpu.VMEM(one, F32)],
        (queries, pos, far, first, middle),
        "score_last",
    )
    parts = lax.all_to_all(parts, COLS, split_axis=0, concat_axis=0, tiled=True)
    loss, ids, pool_emb = merge(parts, pool_emb)
    return (pool_emb, ids.reshape(-1), loss.reshape(-1))


def solution(mesh):
    torus = Mesh(
        mesh.devices.reshape(2, 2, 2, 4, 4), ("rows_0", "rows_1", "cols_0", "cols_1", "cols_2")
    )
    placed = (
        P(ROWS_COLS, None),
        P(),
        P(),
        P(ROWS_COLS),
        P(ROWS_COLS),
        P(ROWS_COLS, None),
        P(ROWS, None),
        P(),
    )
    return jax.shard_map(
        local,
        mesh=torus,
        in_specs=placed,
        out_specs=(P(ROWS_COLS, None), P(ROWS_COLS), P(ROWS)),
        check_vma=False,
    )
```

```python
import math

import jax
import jax.numpy as jnp
from jax import lax
from jax.experimental import pallas as pl
from jax.experimental.pallas import tpu as pltpu
from jax.sharding import Mesh
from jax.sharding import PartitionSpec as P

ROWS = ("rows_0", "rows_1")
COLS = ("cols_0", "cols_1", "cols_2")
ROWS_COLS = ("rows_0", "rows_1", "cols_0", "cols_1", "cols_2")

F32 = jnp.float32
BF16 = jnp.bfloat16
I32 = jnp.int32

N_DEV = 128
N_ROWS = 4
N_COLS = 32
ITEMS = 1024
CAP = 16
EMB = 256
HID = 1024
F_IN = 2048
QDEV = 2048
LANES = 128
BLOCKS = ITEMS // LANES

LOG2E = math.log2(math.e)
LN2 = math.log(2.0)
SCALE2 = 4.0 / math.sqrt(EMB) * LOG2E
FLOOR = -1e30

EXT_SLOTS = ITEMS
EXT_A = EXT_SLOTS + N_DEV // 2
EXT_B = EXT_A + 16
EXT_C = EXT_B + 16
EXT_ROWS = EXT_C + 16

PART_POS = QDEV // LANES
PART_IDS = 2 * PART_POS
PART_ROWS = PART_IDS + 8
N_X = 4
N_PEERS = N_COLS // N_X
X_ROWS = PART_IDS + N_ROWS * N_PEERS

NT = (((1,), (1,)), ((), ()))

K_AT = (0, 256, 1024, F_IN)
K_STEPS = len(K_AT) - 1
ROW_BLOCK = 256


def tower_kernel(
    feat_hbm, w_in_hbm, w_out_hbm, owners_hbm, ids_hbm, counts_hbm,
    ext_ref, send_ref,
    feat, w_in, w_out, acc, owners_ref, ids_ref, counts_ref, slots,
    feat_sem, w_in_sem, w_out_sem, small_sem,
):
    small = [
        pltpu.make_async_copy(held, ref, small_sem.at[k])
        for k, (held, ref) in enumerate(
            ((owners_hbm, owners_ref), (ids_hbm, ids_ref), (counts_hbm, counts_ref))
        )
    ]
    for copy in small:
        copy.start()
    copies = []
    for k in range(K_STEPS):
        at = pl.ds(K_AT[k], K_AT[k + 1] - K_AT[k])
        copies.append(
            (
                pltpu.make_async_copy(w_in_hbm.at[at], w_in.at[at], w_in_sem.at[k]),
                pltpu.make_async_copy(feat_hbm.at[:, at], feat.at[:, at], feat_sem.at[k]),
            )
        )
    w_out_copy = pltpu.make_async_copy(w_out_hbm, w_out, w_out_sem)
    for k in range(2):
        for copy in copies[k]:
            copy.start()

    for copy in small:
        copy.wait()

    owner_iota = lax.broadcasted_iota(I32, (N_DEV, LANES), 0)
    row_iota = lax.broadcasted_iota(I32, (LANES, LANES), 0)
    upper = (row_iota < lax.broadcasted_iota(I32, (LANES, LANES), 1)).astype(F32).astype(BF16)
    seen = jnp.zeros((N_DEV, 1), F32)
    by_slot = jnp.zeros((N_DEV, LANES), F32)
    for j in range(BLOCKS):
        owner = owners_ref[j : j + 1, :]
        onehot = (owner_iota == owner).astype(F32)
        onehot_b = onehot.astype(BF16)
        before = jnp.dot(onehot_b, upper, preferred_element_type=F32) + seen
        rank = jnp.sum(onehot * before, axis=0, keepdims=True).astype(I32)
        seen = seen + jnp.sum(onehot, axis=1, keepdims=True)
        slots[j : j + 1, :] = owner * CAP + rank
        value = ids_ref[j : j + 1, :] + 1
        piece = jnp.where(
            row_iota < CAP,
            value >> 12,
            jnp.where(row_iota < 2 * CAP, (value >> 6) & 63, value & 63),
        )
        here = (row_iota % CAP == rank) & (row_iota < 3 * CAP)
        chosen = jnp.where(here, piece, 0).astype(F32).astype(BF16)
        by_slot = by_slot + lax.dot_general(onehot_b, chosen, NT, preferred_element_type=F32)
    half = N_DEV // 2
    ext_ref[EXT_SLOTS:EXT_A, 0:LANES] = by_slot[0:half, :].astype(BF16)
    ext_ref[EXT_SLOTS:EXT_A, LANES:EMB] = by_slot[half:N_DEV, :].astype(BF16)
    ids = ids_ref[...]
    counts = counts_ref[...]
    none = jnp.zeros((BLOCKS, LANES), I32)
    for at, left, right in (
        (EXT_A, ids >> 12, (ids >> 6) & 63),
        (EXT_B, ids & 63, counts >> 8),
        (EXT_C, counts & 255, none),
    ):
        for lanes, piece in ((slice(0, LANES), left), (slice(LANES, EMB), right)):
            ext_ref[at : at + 16, lanes] = (
                jnp.concatenate([piece, none], axis=0).astype(F32).astype(BF16)
            )

    for k in range(K_STEPS):
        for copy in copies[k]:
            copy.wait()
        if k + 2 < K_STEPS:
            for copy in copies[k + 2]:
                copy.start()
        if k + 2 == K_STEPS:
            w_out_copy.start()
        last = k == K_STEPS - 1
        if last:
            w_out_copy.wait()
        at = slice(K_AT[k], K_AT[k + 1])
        for b in range(ITEMS // ROW_BLOCK):
            rows = slice(b * ROW_BLOCK, (b + 1) * ROW_BLOCK)
            part = jnp.dot(feat[rows, at], w_in[at, :], preferred_element_type=F32)
            if k > 0:
                part = acc[rows, :] + part
            if not last:
                acc[rows, :] = part
            else:
                hidden = jnp.maximum(part, 0.0).astype(BF16)
                ext_ref[rows, :] = jnp.dot(
                    hidden, w_out[...], preferred_element_type=F32
                ).astype(BF16)

    chunk = 512
    slot_row = jnp.concatenate([slots[j : j + 1, :] for j in range(BLOCKS)], axis=1)
    for c in range(N_DEV * CAP // chunk):
        place = lax.broadcasted_iota(I32, (chunk, ITEMS), 0) + c * chunk
        chosen = (place == slot_row).astype(F32).astype(BF16)
        send_ref[c * chunk : (c + 1) * chunk, :] = jnp.dot(
            chosen, ext_ref[0:ITEMS, :], preferred_element_type=F32
        ).astype(BF16)


VMEM_SPEC = pl.BlockSpec(memory_space=pltpu.VMEM)
ANY_SPEC = pl.BlockSpec(memory_space=pl.ANY)


def near_core(value):
    return pltpu.with_memory_space_constraint(value, pltpu.VMEM)


def in_hbm(value):
    return pltpu.with_memory_space_constraint(value, pltpu.HBM)


def tower(features, w_in, w_out, owners, ids, counts):
    return pl.pallas_call(
        tower_kernel,
        in_specs=[ANY_SPEC] * 6,
        out_specs=[VMEM_SPEC, VMEM_SPEC],
        out_shape=[
            pltpu.VMEM((EXT_ROWS, EMB), BF16),
            pltpu.VMEM((N_DEV * CAP, EMB), BF16),
        ],
        scratch_shapes=[
            pltpu.VMEM((ITEMS, F_IN), BF16),
            pltpu.VMEM((F_IN, HID), BF16),
            pltpu.VMEM((HID, EMB), BF16),
            pltpu.VMEM((ITEMS, HID), F32),
            pltpu.VMEM((BLOCKS, LANES), I32),
            pltpu.VMEM((BLOCKS, LANES), I32),
            pltpu.VMEM((BLOCKS, LANES), I32),
            pltpu.VMEM((BLOCKS, LANES), I32),
            pltpu.SemaphoreType.DMA((K_STEPS,)),
            pltpu.SemaphoreType.DMA((K_STEPS,)),
            pltpu.SemaphoreType.DMA,
            pltpu.SemaphoreType.DMA((3,)),
        ],
        cost_estimate=pl.CostEstimate(
            flops=2 * ITEMS * F_IN * HID + 2 * ITEMS * HID * EMB,
            bytes_accessed=2 * (ITEMS * F_IN + F_IN * HID),
            transcendentals=0,
        ),
        compiler_params=pltpu.CompilerParams(vmem_limit_bytes=28 << 20),
        name="tower",
    )(*[in_hbm(a) for a in (features, w_in, w_out, owners, ids, counts)])


Q_TILE = 512
Q_PARTS = Q_TILE // LANES
Q_STEPS = QDEV // Q_TILE
I_TILE = 512
GROUPS = I_TILE // 8
SAMPLE = 16


def row_index():
    return lax.axis_index("rows_0") * 2 + lax.axis_index("rows_1")


def unpack_columns(exts, col_ids, col_logq):
    fill = jnp.zeros((LANES - BLOCKS, LANES), F32)
    for n, ext in enumerate(exts):
        a, b, c = [ext[at : at + 16, :].astype(F32) for at in (EXT_A, EXT_B, EXT_C)]
        a, b, c = a[0:BLOCKS], b[0:BLOCKS], c[0:BLOCKS]
        ids = a[:, 0:LANES] * 4096.0 + a[:, LANES:EMB] * 64.0 + b[:, 0:LANES]
        logq = jnp.log(b[:, LANES:EMB] * 256.0 + c[:, 0:LANES] + 1.0) * LOG2E
        for value, col in ((ids, col_ids), (logq, col_logq)):
            turned = jnp.concatenate([value, fill], axis=0).T
            for j in range(BLOCKS):
                at = n * ITEMS + j * LANES
                col[at : at + LANES, :] = jnp.broadcast_to(turned[:, j : j + 1], (LANES, LANES))


def score_tiles(q_ref, pos_all, row, tiles, exts, col_ids, col_logq, out_ref):
    first, count = tiles
    out_rows = count * Q_PARTS

    def tile_inputs(t):
        q_rows = q_ref[pl.ds(pl.multiple_of(t * Q_TILE, Q_TILE), Q_TILE), :]
        at = row * (QDEV // LANES) + t * Q_PARTS
        pos_row = jnp.concatenate(
            [pos_all[pl.ds(at + u, 1), :].astype(F32) for u in range(Q_PARTS)], axis=1
        )
        return q_rows, jnp.broadcast_to(pos_row, (8, Q_TILE))

    def raw_scores(q_rows, n, c):
        return lax.dot_general(
            exts[n][c * I_TILE : (c + 1) * I_TILE, :], q_rows, NT, preferred_element_type=F32
        )

    def wide(col, at):
        return jnp.concatenate([col[at : at + 8, :]] * Q_PARTS, axis=1)

    def finish(t, top, total, positive):
        highest = jnp.max(top, axis=0, keepdims=True)
        summed = jnp.sum(total * jnp.exp2(top - highest), axis=0, keepdims=True)
        both = (highest + jnp.log(summed) * LOG2E, jnp.sum(positive, axis=0, keepdims=True))
        for k in range(2):
            for u in range(Q_PARTS):
                at = k * out_rows + (t - first) * Q_PARTS + u
                out_ref[pl.ds(at, 1), :] = both[k][:, u * LANES : (u + 1) * LANES]

    chunks = [(n, c) for n in range(len(exts)) for c in range(ITEMS // I_TILE)]

    def fast_tile(t, worst):
        q_rows, pos8 = tile_inputs(t)
        shift = None
        totals = [jnp.zeros((8, Q_TILE), F32)] * 2
        hits = [jnp.full((8, Q_TILE), FLOOR, F32)] * 2
        for n, c in chunks:
            raw = raw_scores(q_rows, n, c)
            if shift is None:
                tops = [jnp.full((8, Q_TILE), FLOOR, F32)] * 2
                for g in range(SAMPLE):
                    logit = raw[g * 8 : g * 8 + 8, :] * SCALE2 - wide(col_logq, g * 8)
                    tops[g % 2] = jnp.maximum(tops[g % 2], logit)
                top = jnp.maximum(tops[0], tops[1])
                shift = jnp.broadcast_to(jnp.max(top, axis=0, keepdims=True), (8, Q_TILE))
            for g in range(GROUPS):
                at = n * ITEMS + c * I_TILE + g * 8
                logit = raw[g * 8 : g * 8 + 8, :] * SCALE2 - wide(col_logq, at) - shift
                totals[g % 2] = totals[g % 2] + jnp.exp2(logit)
                hits[g % 2] = jnp.where(wide(col_ids, at) == pos8, logit, hits[g % 2])
        total = totals[0] + totals[1]
        hit = jnp.maximum(hits[0], hits[1])
        finish(t, shift, total, jnp.where(hit > FLOOR / 2, hit + shift, 0.0))
        return jnp.maximum(worst, total)

    worst = lax.fori_loop(first, first + count, fast_tile, jnp.zeros((8, Q_TILE), F32), unroll=True)

    @pl.when(jnp.logical_not(jnp.max(worst) < 1e37))
    def _():
        def safe_tile(t, _):
            q_rows, pos8 = tile_inputs(t)
            top = jnp.full((8, Q_TILE), FLOOR, F32)
            total = jnp.zeros((8, Q_TILE), F32)
            positive = jnp.zeros((8, Q_TILE), F32)
            for n, c in chunks:
                raw = raw_scores(q_rows, n, c)
                at = slice(n * ITEMS + c * I_TILE, n * ITEMS + (c + 1) * I_TILE)
                logit = raw * SCALE2 - jnp.concatenate([col_logq[at, :]] * Q_PARTS, axis=1)
                match = jnp.concatenate([col_ids[at, :]] * Q_PARTS, axis=1) == pos8[0:1]
                grouped = logit.reshape(GROUPS, 8, Q_TILE)
                new_top = jnp.maximum(top, jnp.max(grouped, axis=0))
                total = total * jnp.exp2(top - new_top) + jnp.sum(
                    jnp.exp2(grouped - new_top[None]), axis=0
                )
                positive = positive + jnp.sum(
                    jnp.where(match, logit, 0.0).reshape(GROUPS, 8, Q_TILE), axis=0
                )
                top = new_top
            finish(t, top, total, positive)
            return 0

        lax.fori_loop(first, first + count, safe_tile, 0)


def slot_ids(held, row):
    shift = (lax.axis_index("cols_1") * 4 + lax.axis_index("cols_2")) % 8 * CAP
    lane = lax.broadcasted_iota(I32, (N_COLS, LANES), 1)
    slots = pl.ds(EXT_SLOTS + (row % 2) * N_COLS, N_COLS)
    piece = jnp.where(
        row >= 2, held[slots, LANES:EMB].astype(F32), held[slots, 0:LANES].astype(F32)
    )
    value = (
        piece * 4096.0
        + pltpu.roll(piece, LANES - CAP, 1) * 64.0
        + pltpu.roll(piece, LANES - 2 * CAP, 1)
        - 1.0
    )
    return pltpu.roll(jnp.where(lane < CAP, value, 0.0), shift, 1)


def score_and_list(q_ref, pos_all, exts, out_ref, col_ids, col_logq):
    row = row_index()
    unpack_columns(exts, col_ids, col_logq)
    for n, ext in enumerate(exts):
        out_ref[PART_IDS + n * N_COLS : PART_IDS + (n + 1) * N_COLS, :] = slot_ids(ext, row)
    score_tiles(q_ref, pos_all, row, (0, Q_STEPS), exts, col_ids, col_logq, out_ref)


def first_kernel(q_ref, pos_all, own, sibling, out_ref, col_ids, col_logq):
    score_and_list(q_ref, pos_all, (own, sibling), out_ref, col_ids, col_logq)


def next_kernel(q_ref, pos_all, across, first, out_ref, col_ids, col_logq):
    del first
    score_and_list(q_ref, pos_all, (across,), out_ref, col_ids, col_logq)


def last_kernel(q_ref, pos_all, far, first, middle, mine, *rest):
    to_x = rest[0 : N_X - 1]
    last, col_ids, col_logq = rest[N_X - 1 :]
    score_and_list(q_ref, pos_all, (far,), last, col_ids, col_logq)
    held = (first, middle, last)
    sums = [ref[0:PART_POS, :] for ref in held]
    highest = jnp.maximum(jnp.maximum(sums[0], sums[1]), sums[2])
    total = sum(jnp.exp2(value - highest) for value in sums)
    positive = sum(ref[PART_POS:PART_IDS, :] for ref in held)
    parts = jnp.concatenate([highest + jnp.log(total) * LOG2E, positive], axis=0)
    row = row_index()
    x = lax.axis_index("cols_1")
    group = N_COLS // 2
    for step, out_ref in enumerate((mine, *to_x)):
        out_ref[0:PART_IDS, :] = parts
        goal = (x + step) % N_X * N_X
        for source, (ref, n) in enumerate(((first, 0), (first, 1), (middle, 0), (last, 0))):
            at = PART_IDS + n * N_COLS
            ids = jnp.concatenate(
                [ref[pl.ds(at + goal, N_X), :], ref[pl.ds(at + group + goal, N_X), :]], axis=0
            )
            out_ref[pl.ds(PART_IDS + (row ^ source) * N_PEERS, N_PEERS), :] = ids


def collect_kernel(mine, *rest):
    out_ref = rest[-1]
    held = (mine, *rest[:-2])
    sums = [ref[0:PART_POS, :] for ref in held]
    highest = sums[0]
    for value in sums[1:]:
        highest = jnp.maximum(highest, value)
    total = sum(jnp.exp2(value - highest) for value in sums)
    positive = sum(ref[PART_POS:PART_IDS, :] for ref in held)
    parts = jnp.concatenate([highest + jnp.log(total) * LOG2E, positive], axis=0)
    out_ref[:, 0:PART_IDS, :] = jnp.broadcast_to(parts[None], (N_PEERS, PART_IDS, LANES))

    x = lax.axis_index("cols_1")
    place = lax.broadcasted_iota(I32, (N_PEERS, 8, LANES), 1)
    found = jnp.zeros((N_PEERS, 8, LANES), F32)
    for step, ref in enumerate(held):
        source = (x + N_X - step) % N_X // 2 * N_ROWS
        for r in range(N_ROWS):
            ids = ref[PART_IDS + r * N_PEERS : PART_IDS + (r + 1) * N_PEERS, :]
            wide = jnp.broadcast_to(ids[:, None, :], (N_PEERS, 8, LANES))
            found = found + jnp.where(place == source + r, wide, 0.0)
    out_ref[:, PART_IDS:PART_ROWS, :] = found


def collect(held):
    return pl.pallas_call(
        collect_kernel,
        in_specs=[VMEM_SPEC] * len(held),
        out_specs=VMEM_SPEC,
        out_shape=pltpu.VMEM((N_PEERS, PART_ROWS, LANES), F32),
        compiler_params=pltpu.CompilerParams(vmem_limit_bytes=8 << 20),
        name="collect",
    )(*[near_core(a) for a in held])


def scored(kernel, n_blocks, out_shapes, scratch, args, name):
    columns = [pltpu.VMEM((n_blocks * ITEMS, LANES), F32)] * 2
    return pl.pallas_call(
        kernel,
        in_specs=[VMEM_SPEC] * len(args),
        out_specs=[VMEM_SPEC] * len(out_shapes),
        out_shape=[pltpu.VMEM(shape, F32) for shape in out_shapes],
        scratch_shapes=scratch + columns,
        cost_estimate=pl.CostEstimate(
            flops=2 * QDEV * n_blocks * ITEMS * EMB,
            bytes_accessed=2 * n_blocks * ITEMS * EMB,
            transcendentals=QDEV * n_blocks * ITEMS,
        ),
        compiler_params=pltpu.CompilerParams(vmem_limit_bytes=20 << 20),
        name=name,
    )(*[near_core(a) for a in args])


def merge_kernel(parts_ref, pool_in, loss_ref, ids_ref, pool_out, sem):
    copy = pltpu.make_async_copy(pool_in, pool_out, sem)
    copy.start()
    part = parts_ref[:, 0:PART_POS, :]
    highest = jnp.max(part, axis=0)
    summed = jnp.sum(jnp.exp2(part - highest[None]), axis=0)
    hit = jnp.sum(parts_ref[:, PART_POS:PART_IDS, :], axis=0)
    loss_ref[...] = jnp.log(summed) + (highest - hit) * LN2
    half = N_PEERS // 2
    for y in range(2):
        found = jnp.sum(parts_ref[y * half : (y + 1) * half, PART_IDS:PART_ROWS, :], axis=0)
        for h in range(2):
            for r in range(N_ROWS):
                at = r * (N_COLS // 8) + y * 2 + h
                ids_ref[at : at + 1, :] = found[h * N_ROWS + r : h * N_ROWS + r + 1, :].astype(I32)
    copy.wait()


def merge(parts, pool):
    return pl.pallas_call(
        merge_kernel,
        in_specs=[VMEM_SPEC, VMEM_SPEC],
        out_specs=[VMEM_SPEC, VMEM_SPEC, ANY_SPEC],
        out_shape=[
            jax.ShapeDtypeStruct((QDEV // LANES, LANES), F32),
            jax.ShapeDtypeStruct((N_DEV * CAP // LANES, LANES), I32),
            pltpu.HBM(pool.shape, pool.dtype),
        ],
        scratch_shapes=[pltpu.SemaphoreType.DMA],
        compiler_params=pltpu.CompilerParams(vmem_limit_bytes=8 << 20),
        name="merge",
    )(near_core(parts), near_core(pool))


SWAP = [(0, 1), (1, 0)]


def local(features, w_in, w_out, item_ids, item_counts, owners, queries, positives):
    pos = positives.reshape(-1, LANES)
    own, send = tower(
        features,
        w_in,
        w_out,
        owners.reshape(BLOCKS, LANES),
        item_ids.reshape(BLOCKS, LANES),
        item_counts.reshape(BLOCKS, LANES),
    )
    across = lax.ppermute(own, "rows_0", SWAP)
    sibling = lax.ppermute(own, "rows_1", SWAP)
    one = (PART_IDS + N_COLS, LANES)
    two = (PART_IDS + 2 * N_COLS, LANES)
    (first,) = scored(first_kernel, 2, [two], [], (queries, pos, own, sibling), "score_first")
    send, _ = lax.optimization_barrier((send, first))
    pool_emb = lax.all_to_all(send, ROWS_COLS, split_axis=0, concat_axis=0, tiled=True)
    far = lax.ppermute(across, "rows_1", SWAP)
    (middle,) = scored(next_kernel, 1, [one], [], (queries, pos, across, first), "score_next")
    mine, *to_x = scored(
        last_kernel,
        1,
        [(X_ROWS, LANES)] * N_X,
        [pltpu.VMEM(one, F32)],
        (queries, pos, far, first, middle),
        "score_last",
    )
    held = [mine] + [
        lax.ppermute(part, "cols_1", [(x, (x + step) % N_X) for x in range(N_X)])
        for step, part in enumerate(to_x, 1)
    ]
    parts = lax.all_to_all(
        collect(held + [pool_emb]), ("cols_0", "cols_2"), split_axis=0, concat_axis=0, tiled=True
    )
    loss, ids, pool_emb = merge(parts, pool_emb)
    return (pool_emb, ids.reshape(-1), loss.reshape(-1))


def solution(mesh):
    torus = Mesh(
        mesh.devices.reshape(2, 2, 2, 4, 4), ("rows_0", "rows_1", "cols_0", "cols_1", "cols_2")
    )
    placed = (
        P(ROWS_COLS, None),
        P(),
        P(),
        P(ROWS_COLS),
        P(ROWS_COLS),
        P(ROWS_COLS, None),
        P(ROWS, None),
        P(),
    )
    return jax.shard_map(
        local,
        mesh=torus,
        in_specs=placed,
        out_specs=(P(ROWS_COLS, None), P(ROWS_COLS), P(ROWS)),
        check_vma=False,
    )
```

```python
import math

import jax
import jax.numpy as jnp
from jax import lax
from jax.experimental import pallas as pl
from jax.experimental.pallas import tpu as pltpu
from jax.sharding import Mesh
from jax.sharding import PartitionSpec as P

ROWS = ("rows_0", "rows_1")
COLS = ("cols_0", "cols_1", "cols_2")
ROWS_COLS = ("rows_0", "rows_1", "cols_0", "cols_1", "cols_2")

F32 = jnp.float32
BF16 = jnp.bfloat16
I32 = jnp.int32

N_DEV = 128
N_ROWS = 4
N_COLS = 32
ITEMS = 1024
CAP = 16
EMB = 256
HID = 1024
F_IN = 2048
QDEV = 2048
LANES = 128
BLOCKS = ITEMS // LANES

LOG2E = math.log2(math.e)
LN2 = math.log(2.0)
SCALE2 = 4.0 / math.sqrt(EMB) * LOG2E
FLOOR = -1e30

EXT_SLOTS = ITEMS
EXT_A = EXT_SLOTS + N_DEV // 2
EXT_B = EXT_A + 16
EXT_C = EXT_B + 16
EXT_ROWS = EXT_C + 16

PART_POS = QDEV // LANES
PART_IDS = 2 * PART_POS
PART_ROWS = PART_IDS + 8
N_X = 4
N_PEERS = N_COLS // N_X
X_ROWS = PART_IDS + N_ROWS * N_PEERS

NT = (((1,), (1,)), ((), ()))

K_AT = (0, 256, 1024, F_IN)
K_STEPS = len(K_AT) - 1
ROW_BLOCK = 256


def tower_kernel(
    feat_hbm, w_in_hbm, w_out_hbm, owners_hbm, ids_hbm, counts_hbm,
    ext_ref, slots,
    feat, w_in, w_out, acc, owners_ref, ids_ref, counts_ref,
    feat_sem, w_in_sem, w_out_sem, small_sem,
):
    small = [
        pltpu.make_async_copy(held, ref, small_sem.at[k])
        for k, (held, ref) in enumerate(
            ((owners_hbm, owners_ref), (ids_hbm, ids_ref), (counts_hbm, counts_ref))
        )
    ]
    for copy in small:
        copy.start()
    copies = []
    for k in range(K_STEPS):
        at = pl.ds(K_AT[k], K_AT[k + 1] - K_AT[k])
        copies.append(
            (
                pltpu.make_async_copy(w_in_hbm.at[at], w_in.at[at], w_in_sem.at[k]),
                pltpu.make_async_copy(feat_hbm.at[:, at], feat.at[:, at], feat_sem.at[k]),
            )
        )
    w_out_copy = pltpu.make_async_copy(w_out_hbm, w_out, w_out_sem)
    for k in range(2):
        for copy in copies[k]:
            copy.start()

    for copy in small:
        copy.wait()

    owner_iota = lax.broadcasted_iota(I32, (N_DEV, LANES), 0)
    row_iota = lax.broadcasted_iota(I32, (LANES, LANES), 0)
    upper = (row_iota < lax.broadcasted_iota(I32, (LANES, LANES), 1)).astype(F32).astype(BF16)
    seen = jnp.zeros((N_DEV, 1), F32)
    by_slot = jnp.zeros((N_DEV, LANES), F32)
    for j in range(BLOCKS):
        owner = owners_ref[j : j + 1, :]
        onehot = (owner_iota == owner).astype(F32)
        onehot_b = onehot.astype(BF16)
        before = jnp.dot(onehot_b, upper, preferred_element_type=F32) + seen
        rank = jnp.sum(onehot * before, axis=0, keepdims=True).astype(I32)
        seen = seen + jnp.sum(onehot, axis=1, keepdims=True)
        slots[j : j + 1, :] = owner * CAP + rank
        value = ids_ref[j : j + 1, :] + 1
        piece = jnp.where(
            row_iota < CAP,
            value >> 12,
            jnp.where(row_iota < 2 * CAP, (value >> 6) & 63, value & 63),
        )
        here = (row_iota % CAP == rank) & (row_iota < 3 * CAP)
        chosen = jnp.where(here, piece, 0).astype(F32).astype(BF16)
        by_slot = by_slot + lax.dot_general(onehot_b, chosen, NT, preferred_element_type=F32)
    half = N_DEV // 2
    ext_ref[EXT_SLOTS:EXT_A, 0:LANES] = by_slot[0:half, :].astype(BF16)
    ext_ref[EXT_SLOTS:EXT_A, LANES:EMB] = by_slot[half:N_DEV, :].astype(BF16)
    ids = ids_ref[...]
    counts = counts_ref[...]
    none = jnp.zeros((BLOCKS, LANES), I32)
    for at, left, right in (
        (EXT_A, ids >> 12, (ids >> 6) & 63),
        (EXT_B, ids & 63, counts >> 8),
        (EXT_C, counts & 255, none),
    ):
        for lanes, piece in ((slice(0, LANES), left), (slice(LANES, EMB), right)):
            ext_ref[at : at + 16, lanes] = (
                jnp.concatenate([piece, none], axis=0).astype(F32).astype(BF16)
            )

    for k in range(K_STEPS):
        for copy in copies[k]:
            copy.wait()
        if k + 2 < K_STEPS:
            for copy in copies[k + 2]:
                copy.start()
        if k + 2 == K_STEPS:
            w_out_copy.start()
        last = k == K_STEPS - 1
        if last:
            w_out_copy.wait()
        at = slice(K_AT[k], K_AT[k + 1])
        for b in range(ITEMS // ROW_BLOCK):
            rows = slice(b * ROW_BLOCK, (b + 1) * ROW_BLOCK)
            part = jnp.dot(feat[rows, at], w_in[at, :], preferred_element_type=F32)
            if k > 0:
                part = acc[rows, :] + part
            if not last:
                acc[rows, :] = part
            else:
                hidden = jnp.maximum(part, 0.0).astype(BF16)
                ext_ref[rows, :] = jnp.dot(
                    hidden, w_out[...], preferred_element_type=F32
                ).astype(BF16)


VMEM_SPEC = pl.BlockSpec(memory_space=pltpu.VMEM)
ANY_SPEC = pl.BlockSpec(memory_space=pl.ANY)


def near_core(value):
    return pltpu.with_memory_space_constraint(value, pltpu.VMEM)


def in_hbm(value):
    return pltpu.with_memory_space_constraint(value, pltpu.HBM)


def tower(features, w_in, w_out, owners, ids, counts):
    return pl.pallas_call(
        tower_kernel,
        in_specs=[ANY_SPEC] * 6,
        out_specs=[VMEM_SPEC, VMEM_SPEC],
        out_shape=[
            pltpu.VMEM((EXT_ROWS, EMB), BF16),
            pltpu.VMEM((BLOCKS, LANES), I32),
        ],
        scratch_shapes=[
            pltpu.VMEM((ITEMS, F_IN), BF16),
            pltpu.VMEM((F_IN, HID), BF16),
            pltpu.VMEM((HID, EMB), BF16),
            pltpu.VMEM((ITEMS, HID), F32),
            pltpu.VMEM((BLOCKS, LANES), I32),
            pltpu.VMEM((BLOCKS, LANES), I32),
            pltpu.VMEM((BLOCKS, LANES), I32),
            pltpu.SemaphoreType.DMA((K_STEPS,)),
            pltpu.SemaphoreType.DMA((K_STEPS,)),
            pltpu.SemaphoreType.DMA,
            pltpu.SemaphoreType.DMA((3,)),
        ],
        cost_estimate=pl.CostEstimate(
            flops=2 * ITEMS * F_IN * HID + 2 * ITEMS * HID * EMB,
            bytes_accessed=2 * (ITEMS * F_IN + F_IN * HID),
            transcendentals=0,
        ),
        compiler_params=pltpu.CompilerParams(vmem_limit_bytes=28 << 20),
        name="tower",
    )(*[in_hbm(a) for a in (features, w_in, w_out, owners, ids, counts)])


Q_TILE = 512
Q_PARTS = Q_TILE // LANES
Q_STEPS = QDEV // Q_TILE
I_TILE = 512
GROUPS = I_TILE // 8
SAMPLE = 16


def row_index():
    return lax.axis_index("rows_0") * 2 + lax.axis_index("rows_1")


def unpack_columns(exts, col_ids, col_logq):
    fill = jnp.zeros((LANES - BLOCKS, LANES), F32)
    for n, ext in enumerate(exts):
        a, b, c = [ext[at : at + 16, :].astype(F32) for at in (EXT_A, EXT_B, EXT_C)]
        a, b, c = a[0:BLOCKS], b[0:BLOCKS], c[0:BLOCKS]
        ids = a[:, 0:LANES] * 4096.0 + a[:, LANES:EMB] * 64.0 + b[:, 0:LANES]
        logq = jnp.log(b[:, LANES:EMB] * 256.0 + c[:, 0:LANES] + 1.0) * LOG2E
        for value, col in ((ids, col_ids), (logq, col_logq)):
            turned = jnp.concatenate([value, fill], axis=0).T
            for j in range(BLOCKS):
                at = n * ITEMS + j * LANES
                col[at : at + LANES, :] = jnp.broadcast_to(turned[:, j : j + 1], (LANES, LANES))


def score_tiles(q_ref, pos_all, row, tiles, exts, col_ids, col_logq, out_ref):
    first, count = tiles
    out_rows = count * Q_PARTS

    def tile_inputs(t):
        q_rows = q_ref[pl.ds(pl.multiple_of(t * Q_TILE, Q_TILE), Q_TILE), :]
        at = row * (QDEV // LANES) + t * Q_PARTS
        pos_row = jnp.concatenate(
            [pos_all[pl.ds(at + u, 1), :].astype(F32) for u in range(Q_PARTS)], axis=1
        )
        return q_rows, jnp.broadcast_to(pos_row, (8, Q_TILE))

    def raw_scores(q_rows, n, c):
        return lax.dot_general(
            exts[n][c * I_TILE : (c + 1) * I_TILE, :], q_rows, NT, preferred_element_type=F32
        )

    def wide(col, at):
        return jnp.concatenate([col[at : at + 8, :]] * Q_PARTS, axis=1)

    def finish(t, top, total, positive):
        highest = jnp.max(top, axis=0, keepdims=True)
        summed = jnp.sum(total * jnp.exp2(top - highest), axis=0, keepdims=True)
        both = (highest + jnp.log(summed) * LOG2E, jnp.sum(positive, axis=0, keepdims=True))
        for k in range(2):
            for u in range(Q_PARTS):
                at = k * out_rows + (t - first) * Q_PARTS + u
                out_ref[pl.ds(at, 1), :] = both[k][:, u * LANES : (u + 1) * LANES]

    chunks = [(n, c) for n in range(len(exts)) for c in range(ITEMS // I_TILE)]

    def fast_tile(t, worst):
        q_rows, pos8 = tile_inputs(t)
        shift = None
        totals = [jnp.zeros((8, Q_TILE), F32)] * 2
        hits = [jnp.full((8, Q_TILE), FLOOR, F32)] * 2
        for n, c in chunks:
            raw = raw_scores(q_rows, n, c)
            if shift is None:
                tops = [jnp.full((8, Q_TILE), FLOOR, F32)] * 2
                for g in range(SAMPLE):
                    logit = raw[g * 8 : g * 8 + 8, :] * SCALE2 - wide(col_logq, g * 8)
                    tops[g % 2] = jnp.maximum(tops[g % 2], logit)
                top = jnp.maximum(tops[0], tops[1])
                shift = jnp.broadcast_to(jnp.max(top, axis=0, keepdims=True), (8, Q_TILE))
            for g in range(GROUPS):
                at = n * ITEMS + c * I_TILE + g * 8
                logit = raw[g * 8 : g * 8 + 8, :] * SCALE2 - wide(col_logq, at) - shift
                totals[g % 2] = totals[g % 2] + jnp.exp2(logit)
                hits[g % 2] = jnp.where(wide(col_ids, at) == pos8, logit, hits[g % 2])
        total = totals[0] + totals[1]
        hit = jnp.maximum(hits[0], hits[1])
        finish(t, shift, total, jnp.where(hit > FLOOR / 2, hit + shift, 0.0))
        return jnp.maximum(worst, total)

    worst = lax.fori_loop(first, first + count, fast_tile, jnp.zeros((8, Q_TILE), F32), unroll=True)

    @pl.when(jnp.logical_not(jnp.max(worst) < 1e37))
    def _():
        def safe_tile(t, _):
            q_rows, pos8 = tile_inputs(t)
            top = jnp.full((8, Q_TILE), FLOOR, F32)
            total = jnp.zeros((8, Q_TILE), F32)
            positive = jnp.zeros((8, Q_TILE), F32)
            for n, c in chunks:
                raw = raw_scores(q_rows, n, c)
                at = slice(n * ITEMS + c * I_TILE, n * ITEMS + (c + 1) * I_TILE)
                logit = raw * SCALE2 - jnp.concatenate([col_logq[at, :]] * Q_PARTS, axis=1)
                match = jnp.concatenate([col_ids[at, :]] * Q_PARTS, axis=1) == pos8[0:1]
                grouped = logit.reshape(GROUPS, 8, Q_TILE)
                new_top = jnp.maximum(top, jnp.max(grouped, axis=0))
                total = total * jnp.exp2(top - new_top) + jnp.sum(
                    jnp.exp2(grouped - new_top[None]), axis=0
                )
                positive = positive + jnp.sum(
                    jnp.where(match, logit, 0.0).reshape(GROUPS, 8, Q_TILE), axis=0
                )
                top = new_top
            finish(t, top, total, positive)
            return 0

        lax.fori_loop(first, first + count, safe_tile, 0)


def slot_ids(held, row):
    shift = (lax.axis_index("cols_1") * 4 + lax.axis_index("cols_2")) % 8 * CAP
    lane = lax.broadcasted_iota(I32, (N_COLS, LANES), 1)
    slots = pl.ds(EXT_SLOTS + (row % 2) * N_COLS, N_COLS)
    piece = jnp.where(
        row >= 2, held[slots, LANES:EMB].astype(F32), held[slots, 0:LANES].astype(F32)
    )
    value = (
        piece * 4096.0
        + pltpu.roll(piece, LANES - CAP, 1) * 64.0
        + pltpu.roll(piece, LANES - 2 * CAP, 1)
        - 1.0
    )
    return pltpu.roll(jnp.where(lane < CAP, value, 0.0), shift, 1)


def score_and_list(q_ref, pos_all, exts, out_ref, col_ids, col_logq):
    row = row_index()
    unpack_columns(exts, col_ids, col_logq)
    for n, ext in enumerate(exts):
        out_ref[PART_IDS + n * N_COLS : PART_IDS + (n + 1) * N_COLS, :] = slot_ids(ext, row)
    score_tiles(q_ref, pos_all, row, (0, Q_STEPS), exts, col_ids, col_logq, out_ref)


SEND_CHUNK = 512
SEND_STEPS = N_DEV * CAP // SEND_CHUNK


def first_kernel(
    q_ref, pos_all, own, sibling, slots, out_ref, send_hbm, send, sems, col_ids, col_logq
):
    slot_row = jnp.concatenate([slots[j : j + 1, :] for j in range(BLOCKS)], axis=1)
    copies = []
    for c in range(SEND_STEPS):
        place = lax.broadcasted_iota(I32, (SEND_CHUNK, ITEMS), 0) + c * SEND_CHUNK
        chosen = (place == slot_row).astype(F32).astype(BF16)
        at = pl.ds(c * SEND_CHUNK, SEND_CHUNK)
        send[at, :] = jnp.dot(
            chosen, own[0:ITEMS, :], preferred_element_type=F32
        ).astype(BF16)
        copies.append(pltpu.make_async_copy(send.at[at], send_hbm.at[at], sems.at[c]))
        copies[c].start()
    score_and_list(q_ref, pos_all, (own, sibling), out_ref, col_ids, col_logq)
    for copy in copies:
        copy.wait()


def next_kernel(q_ref, pos_all, across, first, out_ref, col_ids, col_logq):
    del first
    score_and_list(q_ref, pos_all, (across,), out_ref, col_ids, col_logq)


def last_kernel(q_ref, pos_all, far, first, middle, mine, *rest):
    to_x = rest[0 : N_X - 1]
    last, col_ids, col_logq = rest[N_X - 1 :]
    score_and_list(q_ref, pos_all, (far,), last, col_ids, col_logq)
    held = (first, middle, last)
    sums = [ref[0:PART_POS, :] for ref in held]
    highest = jnp.maximum(jnp.maximum(sums[0], sums[1]), sums[2])
    total = sum(jnp.exp2(value - highest) for value in sums)
    positive = sum(ref[PART_POS:PART_IDS, :] for ref in held)
    parts = jnp.concatenate([highest + jnp.log(total) * LOG2E, positive], axis=0)
    row = row_index()
    x = lax.axis_index("cols_1")
    group = N_COLS // 2
    for step, out_ref in enumerate((mine, *to_x)):
        out_ref[0:PART_IDS, :] = parts
        goal = (x + step) % N_X * N_X
        for source, (ref, n) in enumerate(((first, 0), (first, 1), (middle, 0), (last, 0))):
            at = PART_IDS + n * N_COLS
            ids = jnp.concatenate(
                [ref[pl.ds(at + goal, N_X), :], ref[pl.ds(at + group + goal, N_X), :]], axis=0
            )
            out_ref[pl.ds(PART_IDS + (row ^ source) * N_PEERS, N_PEERS), :] = ids


def collect_kernel(mine, *rest):
    out_ref = rest[-1]
    held = (mine, *rest[:-2])
    sums = [ref[0:PART_POS, :] for ref in held]
    highest = sums[0]
    for value in sums[1:]:
        highest = jnp.maximum(highest, value)
    total = sum(jnp.exp2(value - highest) for value in sums)
    positive = sum(ref[PART_POS:PART_IDS, :] for ref in held)
    parts = jnp.concatenate([highest + jnp.log(total) * LOG2E, positive], axis=0)
    out_ref[:, 0:PART_IDS, :] = jnp.broadcast_to(parts[None], (N_PEERS, PART_IDS, LANES))

    x = lax.axis_index("cols_1")
    place = lax.broadcasted_iota(I32, (N_PEERS, 8, LANES), 1)
    found = jnp.zeros((N_PEERS, 8, LANES), F32)
    for step, ref in enumerate(held):
        source = (x + N_X - step) % N_X // 2 * N_ROWS
        for r in range(N_ROWS):
            ids = ref[PART_IDS + r * N_PEERS : PART_IDS + (r + 1) * N_PEERS, :]
            wide = jnp.broadcast_to(ids[:, None, :], (N_PEERS, 8, LANES))
            found = found + jnp.where(place == source + r, wide, 0.0)
    out_ref[:, PART_IDS:PART_ROWS, :] = found


def collect(held, pool):
    return pl.pallas_call(
        collect_kernel,
        in_specs=[VMEM_SPEC] * (len(held) + 1),
        out_specs=VMEM_SPEC,
        out_shape=pltpu.VMEM((N_PEERS, PART_ROWS, LANES), F32),
        compiler_params=pltpu.CompilerParams(vmem_limit_bytes=8 << 20),
        name="collect",
    )(*[near_core(a) for a in held], near_core(pool))


def scored(kernel, n_blocks, out_shapes, scratch, args, name, in_hbm_too=()):
    columns = [pltpu.VMEM((n_blocks * ITEMS, LANES), F32)] * 2
    return pl.pallas_call(
        kernel,
        in_specs=[VMEM_SPEC] * len(args),
        out_specs=[VMEM_SPEC] * len(out_shapes) + [ANY_SPEC] * len(in_hbm_too),
        out_shape=[pltpu.VMEM(shape, F32) for shape in out_shapes] + list(in_hbm_too),
        scratch_shapes=scratch + columns,
        cost_estimate=pl.CostEstimate(
            flops=2 * QDEV * n_blocks * ITEMS * EMB,
            bytes_accessed=2 * n_blocks * ITEMS * EMB,
            transcendentals=QDEV * n_blocks * ITEMS,
        ),
        compiler_params=pltpu.CompilerParams(vmem_limit_bytes=20 << 20),
        name=name,
    )(*[near_core(a) for a in args])


POOL_STEPS = 8


def merge_kernel(parts_ref, pool_in, loss_ref, ids_ref, pool_out, sems):
    rows = N_DEV * CAP // POOL_STEPS
    copies = []
    for k in range(POOL_STEPS):
        at = pl.ds(k * rows, rows)
        copies.append(pltpu.make_async_copy(pool_in.at[at], pool_out.at[at], sems.at[k]))
        copies[k].start()
    part = parts_ref[:, 0:PART_POS, :]
    highest = jnp.max(part, axis=0)
    summed = jnp.sum(jnp.exp2(part - highest[None]), axis=0)
    hit = jnp.sum(parts_ref[:, PART_POS:PART_IDS, :], axis=0)
    loss_ref[...] = jnp.log(summed) + (highest - hit) * LN2
    half = N_PEERS // 2
    for y in range(2):
        found = jnp.sum(parts_ref[y * half : (y + 1) * half, PART_IDS:PART_ROWS, :], axis=0)
        for h in range(2):
            for r in range(N_ROWS):
                at = r * (N_COLS // 8) + y * 2 + h
                ids_ref[at : at + 1, :] = found[h * N_ROWS + r : h * N_ROWS + r + 1, :].astype(I32)
    for copy in copies:
        copy.wait()


def merge(parts, pool):
    return pl.pallas_call(
        merge_kernel,
        in_specs=[VMEM_SPEC, VMEM_SPEC],
        out_specs=[VMEM_SPEC, VMEM_SPEC, ANY_SPEC],
        out_shape=[
            jax.ShapeDtypeStruct((QDEV // LANES, LANES), F32),
            jax.ShapeDtypeStruct((N_DEV * CAP // LANES, LANES), I32),
            pltpu.HBM(pool.shape, pool.dtype),
        ],
        scratch_shapes=[pltpu.SemaphoreType.DMA((POOL_STEPS,))],
        compiler_params=pltpu.CompilerParams(vmem_limit_bytes=8 << 20),
        name="merge",
    )(near_core(parts), near_core(pool))


SWAP = [(0, 1), (1, 0)]


def local(features, w_in, w_out, item_ids, item_counts, owners, queries, positives):
    pos = positives.reshape(-1, LANES)
    own, slots = tower(
        features,
        w_in,
        w_out,
        owners.reshape(BLOCKS, LANES),
        item_ids.reshape(BLOCKS, LANES),
        item_counts.reshape(BLOCKS, LANES),
    )
    across = lax.ppermute(own, "rows_0", SWAP)
    sibling = lax.ppermute(own, "rows_1", SWAP)
    one = (PART_IDS + N_COLS, LANES)
    two = (PART_IDS + 2 * N_COLS, LANES)
    sent = pltpu.HBM((N_DEV * CAP, EMB), BF16)
    first, send = scored(
        first_kernel,
        2,
        [two],
        [pltpu.VMEM((N_DEV * CAP, EMB), BF16), pltpu.SemaphoreType.DMA((SEND_STEPS,))],
        (queries, pos, own, sibling, slots),
        "score_first",
        [sent],
    )
    pool_emb = lax.all_to_all(send, ROWS_COLS, split_axis=0, concat_axis=0, tiled=True)
    far = lax.ppermute(across, "rows_1", SWAP)
    (middle,) = scored(next_kernel, 1, [one], [], (queries, pos, across, first), "score_next")
    mine, *to_x = scored(
        last_kernel,
        1,
        [(X_ROWS, LANES)] * N_X,
        [pltpu.VMEM(one, F32)],
        (queries, pos, far, first, middle),
        "score_last",
    )
    held = [mine] + [
        lax.ppermute(part, "cols_1", [(x, (x + step) % N_X) for x in range(N_X)])
        for step, part in enumerate(to_x, 1)
    ]
    parts = lax.all_to_all(
        collect(held, pool_emb), ("cols_0", "cols_2"), split_axis=0, concat_axis=0, tiled=True
    )
    loss, ids, pool_emb = merge(parts, pool_emb)
    return (pool_emb, ids.reshape(-1), loss.reshape(-1))


def solution(mesh):
    torus = Mesh(
        mesh.devices.reshape(2, 2, 2, 4, 4), ("rows_0", "rows_1", "cols_0", "cols_1", "cols_2")
    )
    placed = (
        P(ROWS_COLS, None),
        P(),
        P(),
        P(ROWS_COLS),
        P(ROWS_COLS),
        P(ROWS_COLS, None),
        P(ROWS, None),
        P(),
    )
    return jax.shard_map(
        local,
        mesh=torus,
        in_specs=placed,
        out_specs=(P(ROWS_COLS, None), P(ROWS_COLS), P(ROWS)),
        check_vma=False,
    )
```

```python
import math

import jax
import jax.numpy as jnp
from jax import lax
from jax.experimental import pallas as pl
from jax.experimental.pallas import tpu as pltpu
from jax.sharding import Mesh
from jax.sharding import PartitionSpec as P

ROWS = ("rows_0", "rows_1")
COLS = ("cols_0", "cols_1", "cols_2")
ROWS_COLS = ("rows_0", "rows_1", "cols_0", "cols_1", "cols_2")

F32 = jnp.float32
BF16 = jnp.bfloat16
I32 = jnp.int32

N_DEV = 128
N_ROWS = 4
N_COLS = 32
ITEMS = 1024
CAP = 16
EMB = 256
HID = 1024
F_IN = 2048
QDEV = 2048
LANES = 128
BLOCKS = ITEMS // LANES

LOG2E = math.log2(math.e)
LN2 = math.log(2.0)
SCALE2 = 4.0 / math.sqrt(EMB) * LOG2E
FLOOR = -1e30

EXT_SLOTS = ITEMS
EXT_A = EXT_SLOTS + N_DEV // 2
EXT_B = EXT_A + 16
EXT_C = EXT_B + 16
EXT_ROWS = EXT_C + 16

PART_POS = QDEV // LANES
PART_IDS = 2 * PART_POS
PART_ROWS = PART_IDS + 8
N_X = 4
N_PEERS = N_COLS // N_X
X_ROWS = PART_IDS + N_ROWS * N_PEERS

NT = (((1,), (1,)), ((), ()))

K_AT = (0, 256, 1024, F_IN)
K_STEPS = len(K_AT) - 1
ROW_BLOCK = 256


def tower_kernel(
    feat_hbm, w_in_hbm, w_out_hbm, owners_hbm, ids_hbm, counts_hbm,
    ext_ref, slots,
    feat, w_in, w_out, acc, owners_ref, ids_ref, counts_ref,
    feat_sem, w_in_sem, w_out_sem, small_sem,
):
    small = [
        pltpu.make_async_copy(held, ref, small_sem.at[k])
        for k, (held, ref) in enumerate(
            ((owners_hbm, owners_ref), (ids_hbm, ids_ref), (counts_hbm, counts_ref))
        )
    ]
    for copy in small:
        copy.start()
    copies = []
    for k in range(K_STEPS):
        at = pl.ds(K_AT[k], K_AT[k + 1] - K_AT[k])
        copies.append(
            (
                pltpu.make_async_copy(w_in_hbm.at[at], w_in.at[at], w_in_sem.at[k]),
                pltpu.make_async_copy(feat_hbm.at[:, at], feat.at[:, at], feat_sem.at[k]),
            )
        )
    w_out_copy = pltpu.make_async_copy(w_out_hbm, w_out, w_out_sem)
    for k in range(2):
        for copy in copies[k]:
            copy.start()

    for copy in small:
        copy.wait()

    owner_iota = lax.broadcasted_iota(I32, (N_DEV, LANES), 0)
    row_iota = lax.broadcasted_iota(I32, (LANES, LANES), 0)
    upper = (row_iota < lax.broadcasted_iota(I32, (LANES, LANES), 1)).astype(F32).astype(BF16)
    seen = jnp.zeros((N_DEV, 1), F32)
    by_slot = jnp.zeros((N_DEV, LANES), F32)
    for j in range(BLOCKS):
        owner = owners_ref[j : j + 1, :]
        onehot = (owner_iota == owner).astype(F32)
        onehot_b = onehot.astype(BF16)
        before = jnp.dot(onehot_b, upper, preferred_element_type=F32) + seen
        rank = jnp.sum(onehot * before, axis=0, keepdims=True).astype(I32)
        seen = seen + jnp.sum(onehot, axis=1, keepdims=True)
        slots[j : j + 1, :] = owner * CAP + rank
        value = ids_ref[j : j + 1, :] + 1
        piece = jnp.where(
            row_iota < CAP,
            value >> 12,
            jnp.where(row_iota < 2 * CAP, (value >> 6) & 63, value & 63),
        )
        here = (row_iota % CAP == rank) & (row_iota < 3 * CAP)
        chosen = jnp.where(here, piece, 0).astype(F32).astype(BF16)
        by_slot = by_slot + lax.dot_general(onehot_b, chosen, NT, preferred_element_type=F32)
    half = N_DEV // 2
    ext_ref[EXT_SLOTS:EXT_A, 0:LANES] = by_slot[0:half, :].astype(BF16)
    ext_ref[EXT_SLOTS:EXT_A, LANES:EMB] = by_slot[half:N_DEV, :].astype(BF16)
    ids = ids_ref[...]
    counts = counts_ref[...]
    none = jnp.zeros((BLOCKS, LANES), I32)
    for at, left, right in (
        (EXT_A, ids >> 12, (ids >> 6) & 63),
        (EXT_B, ids & 63, counts >> 8),
        (EXT_C, counts & 255, none),
    ):
        for lanes, piece in ((slice(0, LANES), left), (slice(LANES, EMB), right)):
            ext_ref[at : at + 16, lanes] = (
                jnp.concatenate([piece, none], axis=0).astype(F32).astype(BF16)
            )

    for k in range(K_STEPS):
        for copy in copies[k]:
            copy.wait()
        if k + 2 < K_STEPS:
            for copy in copies[k + 2]:
                copy.start()
        if k + 2 == K_STEPS:
            w_out_copy.start()
        last = k == K_STEPS - 1
        if last:
            w_out_copy.wait()
        at = slice(K_AT[k], K_AT[k + 1])
        for b in range(ITEMS // ROW_BLOCK):
            rows = slice(b * ROW_BLOCK, (b + 1) * ROW_BLOCK)
            part = jnp.dot(feat[rows, at], w_in[at, :], preferred_element_type=F32)
            if k > 0:
                part = acc[rows, :] + part
            if not last:
                acc[rows, :] = part
            else:
                hidden = jnp.maximum(part, 0.0).astype(BF16)
                ext_ref[rows, :] = jnp.dot(
                    hidden, w_out[...], preferred_element_type=F32
                ).astype(BF16)


VMEM_SPEC = pl.BlockSpec(memory_space=pltpu.VMEM)
ANY_SPEC = pl.BlockSpec(memory_space=pl.ANY)


def near_core(value):
    return pltpu.with_memory_space_constraint(value, pltpu.VMEM)


def in_hbm(value):
    return pltpu.with_memory_space_constraint(value, pltpu.HBM)


def tower(features, w_in, w_out, owners, ids, counts):
    return pl.pallas_call(
        tower_kernel,
        in_specs=[ANY_SPEC] * 6,
        out_specs=[VMEM_SPEC, VMEM_SPEC],
        out_shape=[
            pltpu.VMEM((EXT_ROWS, EMB), BF16),
            pltpu.VMEM((BLOCKS, LANES), I32),
        ],
        scratch_shapes=[
            pltpu.VMEM((ITEMS, F_IN), BF16),
            pltpu.VMEM((F_IN, HID), BF16),
            pltpu.VMEM((HID, EMB), BF16),
            pltpu.VMEM((ITEMS, HID), F32),
            pltpu.VMEM((BLOCKS, LANES), I32),
            pltpu.VMEM((BLOCKS, LANES), I32),
            pltpu.VMEM((BLOCKS, LANES), I32),
            pltpu.SemaphoreType.DMA((K_STEPS,)),
            pltpu.SemaphoreType.DMA((K_STEPS,)),
            pltpu.SemaphoreType.DMA,
            pltpu.SemaphoreType.DMA((3,)),
        ],
        cost_estimate=pl.CostEstimate(
            flops=2 * ITEMS * F_IN * HID + 2 * ITEMS * HID * EMB,
            bytes_accessed=2 * (ITEMS * F_IN + F_IN * HID),
            transcendentals=0,
        ),
        compiler_params=pltpu.CompilerParams(vmem_limit_bytes=20 << 20),
        name="tower",
    )(*[in_hbm(a) for a in (features, w_in, w_out, owners, ids, counts)])


Q_TILE = 512
Q_PARTS = Q_TILE // LANES
Q_STEPS = QDEV // Q_TILE
I_TILE = 512
GROUPS = I_TILE // 8
SAMPLE = 16


def row_index():
    return lax.axis_index("rows_0") * 2 + lax.axis_index("rows_1")


def unpack_columns(exts, col_ids, col_logq):
    fill = jnp.zeros((LANES - BLOCKS, LANES), F32)
    for n, (ext, skip) in enumerate(exts):
        a, b, c = [
            ext[at - skip : at - skip + 16, :].astype(F32) for at in (EXT_A, EXT_B, EXT_C)
        ]
        a, b, c = a[0:BLOCKS], b[0:BLOCKS], c[0:BLOCKS]
        ids = a[:, 0:LANES] * 4096.0 + a[:, LANES:EMB] * 64.0 + b[:, 0:LANES]
        logq = jnp.log(b[:, LANES:EMB] * 256.0 + c[:, 0:LANES] + 1.0) * LOG2E
        for value, col in ((ids, col_ids), (logq, col_logq)):
            turned = jnp.concatenate([value, fill], axis=0).T
            for j in range(BLOCKS):
                at = n * ITEMS + j * LANES
                col[at : at + LANES, :] = jnp.broadcast_to(turned[:, j : j + 1], (LANES, LANES))


def score_tiles(q_ref, pos_all, row, exts, chunks, col_ids, col_logq, out_ref):
    def tile_inputs(t):
        q_rows = q_ref[pl.ds(pl.multiple_of(t * Q_TILE, Q_TILE), Q_TILE), :]
        at = row * (QDEV // LANES) + t * Q_PARTS
        pos_row = jnp.concatenate(
            [pos_all[pl.ds(at + u, 1), :].astype(F32) for u in range(Q_PARTS)], axis=1
        )
        return q_rows, jnp.broadcast_to(pos_row, (8, Q_TILE))

    def raw_scores(q_rows, n, c):
        ext, skip = exts[n]
        first = c * I_TILE - min(skip, I_TILE)
        return lax.dot_general(
            ext[first : first + I_TILE, :], q_rows, NT, preferred_element_type=F32
        )

    def wide(col, at):
        return jnp.concatenate([col[at : at + 8, :]] * Q_PARTS, axis=1)

    def finish(t, top, total, positive):
        highest = jnp.max(top, axis=0, keepdims=True)
        summed = jnp.sum(total * jnp.exp2(top - highest), axis=0, keepdims=True)
        both = (highest + jnp.log(summed) * LOG2E, jnp.sum(positive, axis=0, keepdims=True))
        for k in range(2):
            for u in range(Q_PARTS):
                at = k * PART_POS + t * Q_PARTS + u
                out_ref[pl.ds(at, 1), :] = both[k][:, u * LANES : (u + 1) * LANES]

    def fast_tile(t, worst):
        q_rows, pos8 = tile_inputs(t)
        shift = None
        totals = [jnp.zeros((8, Q_TILE), F32)] * 2
        hits = [jnp.full((8, Q_TILE), FLOOR, F32)] * 2
        for n, c in chunks:
            raw = raw_scores(q_rows, n, c)
            if shift is None:
                tops = [jnp.full((8, Q_TILE), FLOOR, F32)] * 2
                for g in range(SAMPLE):
                    at = n * ITEMS + c * I_TILE + g * 8
                    logit = raw[g * 8 : g * 8 + 8, :] * SCALE2 - wide(col_logq, at)
                    tops[g % 2] = jnp.maximum(tops[g % 2], logit)
                top = jnp.maximum(tops[0], tops[1])
                shift = jnp.broadcast_to(jnp.max(top, axis=0, keepdims=True), (8, Q_TILE))
            for g in range(GROUPS):
                at = n * ITEMS + c * I_TILE + g * 8
                logit = raw[g * 8 : g * 8 + 8, :] * SCALE2 - wide(col_logq, at) - shift
                totals[g % 2] = totals[g % 2] + jnp.exp2(logit)
                hits[g % 2] = jnp.where(wide(col_ids, at) == pos8, logit, hits[g % 2])
        total = totals[0] + totals[1]
        hit = jnp.maximum(hits[0], hits[1])
        finish(t, shift, total, jnp.where(hit > FLOOR / 2, hit + shift, 0.0))
        return jnp.maximum(worst, total)

    worst = lax.fori_loop(0, Q_STEPS, fast_tile, jnp.zeros((8, Q_TILE), F32), unroll=True)

    @pl.when(jnp.logical_not(jnp.max(worst) < 1e37))
    def _():
        def safe_tile(t, _):
            q_rows, pos8 = tile_inputs(t)
            top = jnp.full((8, Q_TILE), FLOOR, F32)
            total = jnp.zeros((8, Q_TILE), F32)
            positive = jnp.zeros((8, Q_TILE), F32)
            for n, c in chunks:
                raw = raw_scores(q_rows, n, c)
                at = slice(n * ITEMS + c * I_TILE, n * ITEMS + (c + 1) * I_TILE)
                logit = raw * SCALE2 - jnp.concatenate([col_logq[at, :]] * Q_PARTS, axis=1)
                match = jnp.concatenate([col_ids[at, :]] * Q_PARTS, axis=1) == pos8[0:1]
                grouped = logit.reshape(GROUPS, 8, Q_TILE)
                new_top = jnp.maximum(top, jnp.max(grouped, axis=0))
                total = total * jnp.exp2(top - new_top) + jnp.sum(
                    jnp.exp2(grouped - new_top[None]), axis=0
                )
                positive = positive + jnp.sum(
                    jnp.where(match, logit, 0.0).reshape(GROUPS, 8, Q_TILE), axis=0
                )
                top = new_top
            finish(t, top, total, positive)
            return 0

        lax.fori_loop(0, Q_STEPS, safe_tile, 0)


def slot_ids(held, row):
    shift = (lax.axis_index("cols_1") * 4 + lax.axis_index("cols_2")) % 8 * CAP
    lane = lax.broadcasted_iota(I32, (N_COLS, LANES), 1)
    slots = pl.ds(EXT_SLOTS + (row % 2) * N_COLS, N_COLS)
    piece = jnp.where(
        row >= 2, held[slots, LANES:EMB].astype(F32), held[slots, 0:LANES].astype(F32)
    )
    value = (
        piece * 4096.0
        + pltpu.roll(piece, LANES - CAP, 1) * 64.0
        + pltpu.roll(piece, LANES - 2 * CAP, 1)
        - 1.0
    )
    return pltpu.roll(jnp.where(lane < CAP, value, 0.0), shift, 1)


WHOLE = tuple(range(ITEMS // I_TILE))
REST_SKIP = EXT_A - (ITEMS - I_TILE)
REST_ROWS = EXT_ROWS - REST_SKIP


def score_and_list(q_ref, pos_all, exts, chunks, listed, out_ref, col_ids, col_logq):
    row = row_index()
    unpack_columns(exts, col_ids, col_logq)
    for n, ext in enumerate(listed):
        out_ref[PART_IDS + n * N_COLS : PART_IDS + (n + 1) * N_COLS, :] = slot_ids(ext, row)
    score_tiles(q_ref, pos_all, row, exts, chunks, col_ids, col_logq, out_ref)


SEND_CHUNK = 512
SEND_STEPS = N_DEV * CAP // SEND_CHUNK


def first_kernel(
    q_ref, pos_all, own, sibling, slots, out_ref, send_hbm, rest, send, sems, col_ids, col_logq
):
    slot_row = jnp.concatenate([slots[j : j + 1, :] for j in range(BLOCKS)], axis=1)
    copies = []
    for c in range(SEND_STEPS):
        place = lax.broadcasted_iota(I32, (SEND_CHUNK, ITEMS), 0) + c * SEND_CHUNK
        chosen = (place == slot_row).astype(F32).astype(BF16)
        at = pl.ds(c * SEND_CHUNK, SEND_CHUNK)
        send[at, :] = jnp.dot(
            chosen, own[0:ITEMS, :], preferred_element_type=F32
        ).astype(BF16)
        copies.append(pltpu.make_async_copy(send.at[at], send_hbm.at[at], sems.at[c]))
        copies[c].start()
    for k, (at, to, rows) in enumerate(
        ((ITEMS - I_TILE, 0, I_TILE), (EXT_A, I_TILE, EXT_ROWS - EXT_A))
    ):
        copies.append(
            pltpu.make_async_copy(
                sibling.at[pl.ds(at, rows)], rest.at[pl.ds(to, rows)], sems.at[SEND_STEPS + k]
            )
        )
        copies[-1].start()
    both = ((own, 0), (sibling, 0))
    chunks = [(0, c) for c in WHOLE] + [(1, c) for c in WHOLE[:1]]
    score_and_list(q_ref, pos_all, both, chunks, (own, sibling), out_ref, col_ids, col_logq)
    for copy in copies:
        copy.wait()


def next_kernel(q_ref, pos_all, rest, across, first, out_ref, col_ids, col_logq):
    del first
    chunks = [(0, c) for c in WHOLE[1:]] + [(1, c) for c in WHOLE]
    score_and_list(
        q_ref, pos_all, ((rest, REST_SKIP), (across, 0)), chunks, (across,), out_ref, col_ids,
        col_logq,
    )


def last_kernel(q_ref, pos_all, far, first, middle, mine, *rest):
    to_x = rest[0 : N_X - 1]
    last, col_ids, col_logq = rest[N_X - 1 :]
    chunks = [(0, c) for c in WHOLE]
    score_and_list(q_ref, pos_all, ((far, 0),), chunks, (far,), last, col_ids, col_logq)
    held = (first, middle, last)
    sums = [ref[0:PART_POS, :] for ref in held]
    highest = jnp.maximum(jnp.maximum(sums[0], sums[1]), sums[2])
    total = sum(jnp.exp2(value - highest) for value in sums)
    positive = sum(ref[PART_POS:PART_IDS, :] for ref in held)
    parts = jnp.concatenate([highest + jnp.log(total) * LOG2E, positive], axis=0)
    row = row_index()
    x = lax.axis_index("cols_1")
    group = N_COLS // 2
    for step, out_ref in enumerate((mine, *to_x)):
        out_ref[0:PART_IDS, :] = parts
        goal = (x + step) % N_X * N_X
        for source, (ref, n) in enumerate(((first, 0), (first, 1), (middle, 0), (last, 0))):
            at = PART_IDS + n * N_COLS
            ids = jnp.concatenate(
                [ref[pl.ds(at + goal, N_X), :], ref[pl.ds(at + group + goal, N_X), :]], axis=0
            )
            out_ref[pl.ds(PART_IDS + (row ^ source) * N_PEERS, N_PEERS), :] = ids


def collect_kernel(mine, *rest):
    out_ref = rest[-1]
    held = (mine, *rest[:-2])
    sums = [ref[0:PART_POS, :] for ref in held]
    highest = sums[0]
    for value in sums[1:]:
        highest = jnp.maximum(highest, value)
    total = sum(jnp.exp2(value - highest) for value in sums)
    positive = sum(ref[PART_POS:PART_IDS, :] for ref in held)
    parts = jnp.concatenate([highest + jnp.log(total) * LOG2E, positive], axis=0)
    out_ref[:, 0:PART_IDS, :] = jnp.broadcast_to(parts[None], (N_PEERS, PART_IDS, LANES))

    x = lax.axis_index("cols_1")
    place = lax.broadcasted_iota(I32, (N_PEERS, 8, LANES), 1)
    found = jnp.zeros((N_PEERS, 8, LANES), F32)
    for step, ref in enumerate(held):
        source = (x + N_X - step) % N_X // 2 * N_ROWS
        for r in range(N_ROWS):
            ids = ref[PART_IDS + r * N_PEERS : PART_IDS + (r + 1) * N_PEERS, :]
            wide = jnp.broadcast_to(ids[:, None, :], (N_PEERS, 8, LANES))
            found = found + jnp.where(place == source + r, wide, 0.0)
    out_ref[:, PART_IDS:PART_ROWS, :] = found


def collect(held, pool):
    return pl.pallas_call(
        collect_kernel,
        in_specs=[VMEM_SPEC] * (len(held) + 1),
        out_specs=VMEM_SPEC,
        out_shape=pltpu.VMEM((N_PEERS, PART_ROWS, LANES), F32),
        compiler_params=pltpu.CompilerParams(vmem_limit_bytes=8 << 20),
        name="collect",
    )(*[near_core(a) for a in held], near_core(pool))


def scored(kernel, n_blocks, out_shapes, scratch, args, name, in_hbm_too=()):
    columns = [pltpu.VMEM((n_blocks * ITEMS, LANES), F32)] * 2
    return pl.pallas_call(
        kernel,
        in_specs=[VMEM_SPEC] * len(args),
        out_specs=[VMEM_SPEC] * len(out_shapes) + [ANY_SPEC] * len(in_hbm_too),
        out_shape=[pltpu.VMEM(*shape) for shape in out_shapes] + list(in_hbm_too),
        scratch_shapes=scratch + columns,
        cost_estimate=pl.CostEstimate(
            flops=2 * QDEV * n_blocks * ITEMS * EMB,
            bytes_accessed=2 * n_blocks * ITEMS * EMB,
            transcendentals=QDEV * n_blocks * ITEMS,
        ),
        compiler_params=pltpu.CompilerParams(vmem_limit_bytes=12 << 20),
        name=name,
    )(*[near_core(a) if a.shape[0] != REST_ROWS else in_hbm(a) for a in args])


POOL_STEPS = 8


def merge_kernel(parts_ref, pool_in, loss_ref, ids_ref, pool_out, sems):
    rows = N_DEV * CAP // POOL_STEPS
    copies = []
    for k in range(POOL_STEPS):
        at = pl.ds(k * rows, rows)
        copies.append(pltpu.make_async_copy(pool_in.at[at], pool_out.at[at], sems.at[k]))
        copies[k].start()
    part = parts_ref[:, 0:PART_POS, :]
    highest = jnp.max(part, axis=0)
    summed = jnp.sum(jnp.exp2(part - highest[None]), axis=0)
    hit = jnp.sum(parts_ref[:, PART_POS:PART_IDS, :], axis=0)
    loss_ref[...] = jnp.log(summed) + (highest - hit) * LN2
    half = N_PEERS // 2
    for y in range(2):
        found = jnp.sum(parts_ref[y * half : (y + 1) * half, PART_IDS:PART_ROWS, :], axis=0)
        for h in range(2):
            for r in range(N_ROWS):
                at = r * (N_COLS // 8) + y * 2 + h
                ids_ref[at : at + 1, :] = found[h * N_ROWS + r : h * N_ROWS + r + 1, :].astype(I32)
    for copy in copies:
        copy.wait()


def merge(parts, pool):
    return pl.pallas_call(
        merge_kernel,
        in_specs=[VMEM_SPEC, VMEM_SPEC],
        out_specs=[VMEM_SPEC, VMEM_SPEC, ANY_SPEC],
        out_shape=[
            jax.ShapeDtypeStruct((QDEV // LANES, LANES), F32),
            jax.ShapeDtypeStruct((N_DEV * CAP // LANES, LANES), I32),
            pltpu.HBM(pool.shape, pool.dtype),
        ],
        scratch_shapes=[pltpu.SemaphoreType.DMA((POOL_STEPS,))],
        compiler_params=pltpu.CompilerParams(vmem_limit_bytes=8 << 20),
        name="merge",
    )(near_core(parts), near_core(pool))


SWAP = [(0, 1), (1, 0)]


def local(features, w_in, w_out, item_ids, item_counts, owners, queries, positives):
    pos = positives.reshape(-1, LANES)
    own, slots = tower(
        features,
        w_in,
        w_out,
        owners.reshape(BLOCKS, LANES),
        item_ids.reshape(BLOCKS, LANES),
        item_counts.reshape(BLOCKS, LANES),
    )
    across = lax.ppermute(own, "rows_0", SWAP)
    sibling = lax.ppermute(own, "rows_1", SWAP)
    one = ((PART_IDS + N_COLS, LANES), F32)
    two = ((PART_IDS + 2 * N_COLS, LANES), F32)
    sent = pltpu.HBM((N_DEV * CAP, EMB), BF16)
    first, send, rest = scored(
        first_kernel,
        2,
        [two],
        [pltpu.VMEM((N_DEV * CAP, EMB), BF16), pltpu.SemaphoreType.DMA((SEND_STEPS + 2,))],
        (queries, pos, own, sibling, slots),
        "score_first",
        [sent, pltpu.HBM((REST_ROWS, EMB), BF16)],
    )
    pool_emb = lax.all_to_all(send, ROWS_COLS, split_axis=0, concat_axis=0, tiled=True)
    far = lax.ppermute(across, "rows_1", SWAP)
    (middle,) = scored(
        next_kernel, 2, [one], [], (queries, pos, rest, across, first), "score_next"
    )
    mine, *to_x = scored(
        last_kernel,
        1,
        [((X_ROWS, LANES), F32)] * N_X,
        [pltpu.VMEM(*one)],
        (queries, pos, far, first, middle),
        "score_last",
    )
    held = [mine] + [
        lax.ppermute(part, "cols_1", [(x, (x + step) % N_X) for x in range(N_X)])
        for step, part in enumerate(to_x, 1)
    ]
    parts = lax.all_to_all(
        collect(held, pool_emb), ("cols_0", "cols_2"), split_axis=0, concat_axis=0, tiled=True
    )
    loss, ids, pool_emb = merge(parts, pool_emb)
    return (pool_emb, ids.reshape(-1), loss.reshape(-1))


def solution(mesh):
    torus = Mesh(
        mesh.devices.reshape(2, 2, 2, 4, 4), ("rows_0", "rows_1", "cols_0", "cols_1", "cols_2")
    )
    placed = (
        P(ROWS_COLS, None),
        P(),
        P(),
        P(ROWS_COLS),
        P(ROWS_COLS),
        P(ROWS_COLS, None),
        P(ROWS, None),
        P(),
    )
    return jax.shard_map(
        local,
        mesh=torus,
        in_specs=placed,
        out_specs=(P(ROWS_COLS, None), P(ROWS_COLS), P(ROWS)),
        check_vma=False,
    )
```

```python
import math

import jax
import jax.numpy as jnp
from jax import lax
from jax.experimental import pallas as pl
from jax.experimental.pallas import tpu as pltpu
from jax.sharding import Mesh
from jax.sharding import PartitionSpec as P

ROWS = ("rows_0", "rows_1")
COLS = ("cols_0", "cols_1", "cols_2")
ROWS_COLS = ("rows_0", "rows_1", "cols_0", "cols_1", "cols_2")

F32 = jnp.float32
BF16 = jnp.bfloat16
I32 = jnp.int32

N_DEV = 128
N_ROWS = 4
N_COLS = 32
ITEMS = 1024
CAP = 16
EMB = 256
HID = 1024
F_IN = 2048
QDEV = 2048
LANES = 128
BLOCKS = ITEMS // LANES

LOG2E = math.log2(math.e)
LN2 = math.log(2.0)
SCALE2 = 4.0 / math.sqrt(EMB) * LOG2E
FLOOR = -1e30

EXT_SLOTS = ITEMS
EXT_A = EXT_SLOTS + N_DEV // 2
EXT_B = EXT_A + 16
EXT_C = EXT_B + 16
EXT_ROWS = EXT_C + 16

PART_POS = QDEV // LANES
PART_IDS = 2 * PART_POS
PART_ROWS = PART_IDS + 8
N_X = 4
N_PEERS = N_COLS // N_X
X_ROWS = PART_IDS + N_ROWS * N_PEERS

NT = (((1,), (1,)), ((), ()))

K_AT = (0, 256, 1024, F_IN)
K_STEPS = len(K_AT) - 1
ROW_BLOCK = 256


def tower_kernel(
    feat_hbm, w_in_hbm, w_out_hbm, owners_hbm, ids_hbm, counts_hbm,
    ext_ref, slots,
    feat, w_in, w_out, acc, owners_ref, ids_ref, counts_ref,
    feat_sem, w_in_sem, w_out_sem, small_sem,
):
    small = [
        pltpu.make_async_copy(held, ref, small_sem.at[k])
        for k, (held, ref) in enumerate(
            ((owners_hbm, owners_ref), (ids_hbm, ids_ref), (counts_hbm, counts_ref))
        )
    ]
    for copy in small:
        copy.start()
    copies = []
    for k in range(K_STEPS):
        at = pl.ds(K_AT[k], K_AT[k + 1] - K_AT[k])
        copies.append(
            (
                pltpu.make_async_copy(w_in_hbm.at[at], w_in.at[at], w_in_sem.at[k]),
                pltpu.make_async_copy(feat_hbm.at[:, at], feat.at[:, at], feat_sem.at[k]),
            )
        )
    w_out_copy = pltpu.make_async_copy(w_out_hbm, w_out, w_out_sem)
    for k in range(2):
        for copy in copies[k]:
            copy.start()

    for copy in small:
        copy.wait()

    owner_iota = lax.broadcasted_iota(I32, (N_DEV, LANES), 0)
    row_iota = lax.broadcasted_iota(I32, (LANES, LANES), 0)
    upper = (row_iota < lax.broadcasted_iota(I32, (LANES, LANES), 1)).astype(F32).astype(BF16)
    seen = jnp.zeros((N_DEV, 1), F32)
    by_slot = jnp.zeros((N_DEV, LANES), F32)
    for j in range(BLOCKS):
        owner = owners_ref[j : j + 1, :]
        onehot = (owner_iota == owner).astype(F32)
        onehot_b = onehot.astype(BF16)
        before = jnp.dot(onehot_b, upper, preferred_element_type=F32) + seen
        rank = jnp.sum(onehot * before, axis=0, keepdims=True).astype(I32)
        seen = seen + jnp.sum(onehot, axis=1, keepdims=True)
        slots[j : j + 1, :] = owner * CAP + rank
        value = ids_ref[j : j + 1, :] + 1
        piece = jnp.where(
            row_iota < CAP,
            value >> 12,
            jnp.where(row_iota < 2 * CAP, (value >> 6) & 63, value & 63),
        )
        here = (row_iota % CAP == rank) & (row_iota < 3 * CAP)
        chosen = jnp.where(here, piece, 0).astype(F32).astype(BF16)
        by_slot = by_slot + lax.dot_general(onehot_b, chosen, NT, preferred_element_type=F32)
    half = N_DEV // 2
    ext_ref[EXT_SLOTS:EXT_A, 0:LANES] = by_slot[0:half, :].astype(BF16)
    ext_ref[EXT_SLOTS:EXT_A, LANES:EMB] = by_slot[half:N_DEV, :].astype(BF16)
    ids = ids_ref[...]
    counts = counts_ref[...]
    none = jnp.zeros((BLOCKS, LANES), I32)
    for at, left, right in (
        (EXT_A, ids >> 12, (ids >> 6) & 63),
        (EXT_B, ids & 63, counts >> 8),
        (EXT_C, counts & 255, none),
    ):
        for lanes, piece in ((slice(0, LANES), left), (slice(LANES, EMB), right)):
            ext_ref[at : at + 16, lanes] = (
                jnp.concatenate([piece, none], axis=0).astype(F32).astype(BF16)
            )

    for k in range(K_STEPS):
        for copy in copies[k]:
            copy.wait()
        if k + 2 < K_STEPS:
            for copy in copies[k + 2]:
                copy.start()
        if k + 2 == K_STEPS:
            w_out_copy.start()
        last = k == K_STEPS - 1
        if last:
            w_out_copy.wait()
        at = slice(K_AT[k], K_AT[k + 1])
        for b in range(ITEMS // ROW_BLOCK):
            rows = slice(b * ROW_BLOCK, (b + 1) * ROW_BLOCK)
            part = jnp.dot(feat[rows, at], w_in[at, :], preferred_element_type=F32)
            if k > 0:
                part = acc[rows, :] + part
            if not last:
                acc[rows, :] = part
            else:
                hidden = jnp.maximum(part, 0.0).astype(BF16)
                ext_ref[rows, :] = jnp.dot(
                    hidden, w_out[...], preferred_element_type=F32
                ).astype(BF16)


VMEM_SPEC = pl.BlockSpec(memory_space=pltpu.VMEM)
ANY_SPEC = pl.BlockSpec(memory_space=pl.ANY)


def near_core(value):
    return pltpu.with_memory_space_constraint(value, pltpu.VMEM)


def in_hbm(value):
    return pltpu.with_memory_space_constraint(value, pltpu.HBM)


def tower(features, w_in, w_out, owners, ids, counts):
    return pl.pallas_call(
        tower_kernel,
        in_specs=[ANY_SPEC] * 6,
        out_specs=[VMEM_SPEC, VMEM_SPEC],
        out_shape=[
            pltpu.VMEM((EXT_ROWS, EMB), BF16),
            pltpu.VMEM((BLOCKS, LANES), I32),
        ],
        scratch_shapes=[
            pltpu.VMEM((ITEMS, F_IN), BF16),
            pltpu.VMEM((F_IN, HID), BF16),
            pltpu.VMEM((HID, EMB), BF16),
            pltpu.VMEM((ITEMS, HID), F32),
            pltpu.VMEM((BLOCKS, LANES), I32),
            pltpu.VMEM((BLOCKS, LANES), I32),
            pltpu.VMEM((BLOCKS, LANES), I32),
            pltpu.SemaphoreType.DMA((K_STEPS,)),
            pltpu.SemaphoreType.DMA((K_STEPS,)),
            pltpu.SemaphoreType.DMA,
            pltpu.SemaphoreType.DMA((3,)),
        ],
        cost_estimate=pl.CostEstimate(
            flops=2 * ITEMS * F_IN * HID + 2 * ITEMS * HID * EMB,
            bytes_accessed=2 * (ITEMS * F_IN + F_IN * HID),
            transcendentals=0,
        ),
        compiler_params=pltpu.CompilerParams(vmem_limit_bytes=20 << 20),
        name="tower",
    )(*[in_hbm(a) for a in (features, w_in, w_out, owners, ids, counts)])


Q_TILE = 512
Q_PARTS = Q_TILE // LANES
Q_STEPS = QDEV // Q_TILE
I_TILE = 512
GROUPS = I_TILE // 8
SAMPLE = 4


def row_index():
    return lax.axis_index("rows_0") * 2 + lax.axis_index("rows_1")


def unpack_columns(exts, chunks, col_ids, col_logq):
    fill = jnp.zeros((LANES - BLOCKS, LANES), F32)
    for n, (ext, skip) in enumerate(exts):
        a, b, c = [
            ext[at - skip : at - skip + 16, :].astype(F32) for at in (EXT_A, EXT_B, EXT_C)
        ]
        a, b, c = a[0:BLOCKS], b[0:BLOCKS], c[0:BLOCKS]
        ids = a[:, 0:LANES] * 4096.0 + a[:, LANES:EMB] * 64.0 + b[:, 0:LANES]
        logq = jnp.log(b[:, LANES:EMB] * 256.0 + c[:, 0:LANES] + 1.0) * LOG2E
        for value, col in ((ids, col_ids), (logq, col_logq)):
            turned = jnp.concatenate([value, fill], axis=0).T
            for j in range(BLOCKS):
                if (n, j * LANES // I_TILE) not in chunks:
                    continue
                at = n * ITEMS + j * LANES
                col[at : at + LANES, :] = jnp.broadcast_to(turned[:, j : j + 1], (LANES, LANES))


def score_tiles(q_ref, pos_all, row, exts, chunks, col_ids, col_logq, out_ref):
    def tile_inputs(t):
        q_rows = q_ref[pl.ds(pl.multiple_of(t * Q_TILE, Q_TILE), Q_TILE), :]
        at = row * (QDEV // LANES) + t * Q_PARTS
        pos_row = jnp.concatenate(
            [pos_all[pl.ds(at + u, 1), :].astype(F32) for u in range(Q_PARTS)], axis=1
        )
        return q_rows, jnp.broadcast_to(pos_row, (8, Q_TILE))

    def raw_scores(q_rows, n, c):
        ext, skip = exts[n]
        first = c * I_TILE - min(skip, I_TILE)
        return lax.dot_general(
            ext[first : first + I_TILE, :], q_rows, NT, preferred_element_type=F32
        )

    def wide(col, at):
        return jnp.concatenate([col[at : at + 8, :]] * Q_PARTS, axis=1)

    def finish(t, top, total, positive):
        highest = jnp.max(top, axis=0, keepdims=True)
        summed = jnp.sum(total * jnp.exp2(top - highest), axis=0, keepdims=True)
        both = (highest + jnp.log(summed) * LOG2E, jnp.sum(positive, axis=0, keepdims=True))
        for k in range(2):
            for u in range(Q_PARTS):
                at = k * PART_POS + t * Q_PARTS + u
                out_ref[pl.ds(at, 1), :] = both[k][:, u * LANES : (u + 1) * LANES]

    def fast_tile(t, worst):
        q_rows, pos8 = tile_inputs(t)
        shift = None
        totals = [jnp.zeros((8, Q_TILE), F32)] * 2
        hits = [jnp.full((8, Q_TILE), FLOOR, F32)] * 2
        for n, c in chunks:
            raw = raw_scores(q_rows, n, c)
            if shift is None:
                tops = [jnp.full((8, Q_TILE), FLOOR, F32)] * 2
                for g in range(SAMPLE):
                    at = n * ITEMS + c * I_TILE + g * 8
                    logit = raw[g * 8 : g * 8 + 8, :] * SCALE2 - wide(col_logq, at)
                    tops[g % 2] = jnp.maximum(tops[g % 2], logit)
                top = jnp.maximum(tops[0], tops[1])
                shift = jnp.broadcast_to(jnp.max(top, axis=0, keepdims=True), (8, Q_TILE))
            for g in range(GROUPS):
                at = n * ITEMS + c * I_TILE + g * 8
                logit = raw[g * 8 : g * 8 + 8, :] * SCALE2 - wide(col_logq, at) - shift
                totals[g % 2] = totals[g % 2] + jnp.exp2(logit)
                hits[g % 2] = jnp.where(wide(col_ids, at) == pos8, logit, hits[g % 2])
        total = totals[0] + totals[1]
        hit = jnp.maximum(hits[0], hits[1])
        finish(t, shift, total, jnp.where(hit > FLOOR / 2, hit + shift, 0.0))
        return jnp.maximum(worst, total)

    worst = lax.fori_loop(0, Q_STEPS, fast_tile, jnp.zeros((8, Q_TILE), F32), unroll=True)

    @pl.when(jnp.logical_not(jnp.max(worst) < 1e37))
    def _():
        def safe_tile(t, _):
            q_rows, pos8 = tile_inputs(t)
            top = jnp.full((8, Q_TILE), FLOOR, F32)
            total = jnp.zeros((8, Q_TILE), F32)
            positive = jnp.zeros((8, Q_TILE), F32)
            for n, c in chunks:
                raw = raw_scores(q_rows, n, c)
                at = slice(n * ITEMS + c * I_TILE, n * ITEMS + (c + 1) * I_TILE)
                logit = raw * SCALE2 - jnp.concatenate([col_logq[at, :]] * Q_PARTS, axis=1)
                match = jnp.concatenate([col_ids[at, :]] * Q_PARTS, axis=1) == pos8[0:1]
                grouped = logit.reshape(GROUPS, 8, Q_TILE)
                new_top = jnp.maximum(top, jnp.max(grouped, axis=0))
                total = total * jnp.exp2(top - new_top) + jnp.sum(
                    jnp.exp2(grouped - new_top[None]), axis=0
                )
                positive = positive + jnp.sum(
                    jnp.where(match, logit, 0.0).reshape(GROUPS, 8, Q_TILE), axis=0
                )
                top = new_top
            finish(t, top, total, positive)
            return 0

        lax.fori_loop(0, Q_STEPS, safe_tile, 0)


def slot_ids(held, row):
    shift = (lax.axis_index("cols_1") * 4 + lax.axis_index("cols_2")) % 8 * CAP
    lane = lax.broadcasted_iota(I32, (N_COLS, LANES), 1)
    slots = pl.ds(EXT_SLOTS + (row % 2) * N_COLS, N_COLS)
    piece = jnp.where(
        row >= 2, held[slots, LANES:EMB].astype(F32), held[slots, 0:LANES].astype(F32)
    )
    value = (
        piece * 4096.0
        + pltpu.roll(piece, LANES - CAP, 1) * 64.0
        + pltpu.roll(piece, LANES - 2 * CAP, 1)
        - 1.0
    )
    return pltpu.roll(jnp.where(lane < CAP, value, 0.0), shift, 1)


WHOLE = tuple(range(ITEMS // I_TILE))
REST_SKIP = EXT_A - (ITEMS - I_TILE)
REST_ROWS = EXT_ROWS - REST_SKIP


def score_and_list(q_ref, pos_all, exts, chunks, listed, out_ref, col_ids, col_logq):
    row = row_index()
    unpack_columns(exts, chunks, col_ids, col_logq)
    for n, ext in enumerate(listed):
        out_ref[PART_IDS + n * N_COLS : PART_IDS + (n + 1) * N_COLS, :] = slot_ids(ext, row)
    score_tiles(q_ref, pos_all, row, exts, chunks, col_ids, col_logq, out_ref)


SEND_CHUNK = 512
SEND_STEPS = N_DEV * CAP // SEND_CHUNK


def first_kernel(
    q_ref, pos_all, own, sibling, slots, out_ref, send_hbm, rest, send, sems, col_ids, col_logq
):
    slot_row = jnp.concatenate([slots[j : j + 1, :] for j in range(BLOCKS)], axis=1)
    copies = []
    for c in range(SEND_STEPS):
        place = lax.broadcasted_iota(I32, (SEND_CHUNK, ITEMS), 0) + c * SEND_CHUNK
        chosen = (place == slot_row).astype(F32).astype(BF16)
        at = pl.ds(c * SEND_CHUNK, SEND_CHUNK)
        send[at, :] = jnp.dot(
            chosen, own[0:ITEMS, :], preferred_element_type=F32
        ).astype(BF16)
        copies.append(pltpu.make_async_copy(send.at[at], send_hbm.at[at], sems.at[c]))
        copies[c].start()
    for k, (at, to, rows) in enumerate(
        ((ITEMS - I_TILE, 0, I_TILE), (EXT_A, I_TILE, EXT_ROWS - EXT_A))
    ):
        copies.append(
            pltpu.make_async_copy(
                sibling.at[pl.ds(at, rows)], rest.at[pl.ds(to, rows)], sems.at[SEND_STEPS + k]
            )
        )
        copies[-1].start()
    both = ((own, 0), (sibling, 0))
    chunks = [(0, c) for c in WHOLE] + [(1, c) for c in WHOLE[:1]]
    score_and_list(q_ref, pos_all, both, chunks, (own, sibling), out_ref, col_ids, col_logq)
    for copy in copies:
        copy.wait()


def next_kernel(q_ref, pos_all, rest, across, first, out_ref, col_ids, col_logq):
    del first
    chunks = [(0, c) for c in WHOLE[1:]] + [(1, c) for c in WHOLE]
    score_and_list(
        q_ref, pos_all, ((rest, REST_SKIP), (across, 0)), chunks, (across,), out_ref, col_ids,
        col_logq,
    )


def last_kernel(q_ref, pos_all, far, first, middle, mine, *rest):
    to_x = rest[0 : N_X - 1]
    last, col_ids, col_logq = rest[N_X - 1 :]
    chunks = [(0, c) for c in WHOLE]
    score_and_list(q_ref, pos_all, ((far, 0),), chunks, (far,), last, col_ids, col_logq)
    held = (first, middle, last)
    sums = [ref[0:PART_POS, :] for ref in held]
    highest = jnp.maximum(jnp.maximum(sums[0], sums[1]), sums[2])
    total = sum(jnp.exp2(value - highest) for value in sums)
    positive = sum(ref[PART_POS:PART_IDS, :] for ref in held)
    parts = jnp.concatenate([highest + jnp.log(total) * LOG2E, positive], axis=0)
    row = row_index()
    x = lax.axis_index("cols_1")
    group = N_COLS // 2
    for step, out_ref in enumerate((mine, *to_x)):
        out_ref[0:PART_IDS, :] = parts
        goal = (x + step) % N_X * N_X
        for source, (ref, n) in enumerate(((first, 0), (first, 1), (middle, 0), (last, 0))):
            at = PART_IDS + n * N_COLS
            ids = jnp.concatenate(
                [ref[pl.ds(at + goal, N_X), :], ref[pl.ds(at + group + goal, N_X), :]], axis=0
            )
            out_ref[pl.ds(PART_IDS + (row ^ source) * N_PEERS, N_PEERS), :] = ids


def collect_kernel(mine, *rest):
    out_ref = rest[-1]
    held = (mine, *rest[:-2])
    sums = [ref[0:PART_POS, :] for ref in held]
    highest = sums[0]
    for value in sums[1:]:
        highest = jnp.maximum(highest, value)
    total = sum(jnp.exp2(value - highest) for value in sums)
    positive = sum(ref[PART_POS:PART_IDS, :] for ref in held)
    parts = jnp.concatenate([highest + jnp.log(total) * LOG2E, positive], axis=0)
    out_ref[:, 0:PART_IDS, :] = jnp.broadcast_to(parts[None], (N_PEERS, PART_IDS, LANES))

    x = lax.axis_index("cols_1")
    place = lax.broadcasted_iota(I32, (N_PEERS, 8, LANES), 1)
    found = jnp.zeros((N_PEERS, 8, LANES), F32)
    for step, ref in enumerate(held):
        source = (x + N_X - step) % N_X // 2 * N_ROWS
        for r in range(N_ROWS):
            ids = ref[PART_IDS + r * N_PEERS : PART_IDS + (r + 1) * N_PEERS, :]
            wide = jnp.broadcast_to(ids[:, None, :], (N_PEERS, 8, LANES))
            found = found + jnp.where(place == source + r, wide, 0.0)
    out_ref[:, PART_IDS:PART_ROWS, :] = found


def collect(held, pool):
    return pl.pallas_call(
        collect_kernel,
        in_specs=[VMEM_SPEC] * (len(held) + 1),
        out_specs=VMEM_SPEC,
        out_shape=pltpu.VMEM((N_PEERS, PART_ROWS, LANES), F32),
        compiler_params=pltpu.CompilerParams(vmem_limit_bytes=8 << 20),
        name="collect",
    )(*[near_core(a) for a in held], near_core(pool))


def scored(kernel, n_blocks, out_shapes, scratch, args, name, in_hbm_too=()):
    columns = [pltpu.VMEM((n_blocks * ITEMS, LANES), F32)] * 2
    return pl.pallas_call(
        kernel,
        in_specs=[VMEM_SPEC] * len(args),
        out_specs=[VMEM_SPEC] * len(out_shapes) + [ANY_SPEC] * len(in_hbm_too),
        out_shape=[pltpu.VMEM(*shape) for shape in out_shapes] + list(in_hbm_too),
        scratch_shapes=scratch + columns,
        cost_estimate=pl.CostEstimate(
            flops=2 * QDEV * n_blocks * ITEMS * EMB,
            bytes_accessed=2 * n_blocks * ITEMS * EMB,
            transcendentals=QDEV * n_blocks * ITEMS,
        ),
        compiler_params=pltpu.CompilerParams(vmem_limit_bytes=12 << 20),
        name=name,
    )(*[near_core(a) if a.shape[0] != REST_ROWS else in_hbm(a) for a in args])


POOL_STEPS = 8


def merge_kernel(parts_ref, pool_in, loss_ref, ids_ref, pool_out, sems):
    rows = N_DEV * CAP // POOL_STEPS
    copies = []
    for k in range(POOL_STEPS):
        at = pl.ds(k * rows, rows)
        copies.append(pltpu.make_async_copy(pool_in.at[at], pool_out.at[at], sems.at[k]))
        copies[k].start()
    part = parts_ref[:, 0:PART_POS, :]
    highest = jnp.max(part, axis=0)
    summed = jnp.sum(jnp.exp2(part - highest[None]), axis=0)
    hit = jnp.sum(parts_ref[:, PART_POS:PART_IDS, :], axis=0)
    loss_ref[...] = jnp.log(summed) + (highest - hit) * LN2
    half = N_PEERS // 2
    for y in range(2):
        found = jnp.sum(parts_ref[y * half : (y + 1) * half, PART_IDS:PART_ROWS, :], axis=0)
        for h in range(2):
            for r in range(N_ROWS):
                at = r * (N_COLS // 8) + y * 2 + h
                ids_ref[at : at + 1, :] = found[h * N_ROWS + r : h * N_ROWS + r + 1, :].astype(I32)
    for copy in copies:
        copy.wait()


def merge(parts, pool):
    return pl.pallas_call(
        merge_kernel,
        in_specs=[VMEM_SPEC, VMEM_SPEC],
        out_specs=[VMEM_SPEC, VMEM_SPEC, ANY_SPEC],
        out_shape=[
            jax.ShapeDtypeStruct((QDEV // LANES, LANES), F32),
            jax.ShapeDtypeStruct((N_DEV * CAP // LANES, LANES), I32),
            pltpu.HBM(pool.shape, pool.dtype),
        ],
        scratch_shapes=[pltpu.SemaphoreType.DMA((POOL_STEPS,))],
        compiler_params=pltpu.CompilerParams(vmem_limit_bytes=8 << 20),
        name="merge",
    )(near_core(parts), near_core(pool))


SWAP = [(0, 1), (1, 0)]


def local(features, w_in, w_out, item_ids, item_counts, owners, queries, positives):
    pos = positives.reshape(-1, LANES)
    own, slots = tower(
        features,
        w_in,
        w_out,
        owners.reshape(BLOCKS, LANES),
        item_ids.reshape(BLOCKS, LANES),
        item_counts.reshape(BLOCKS, LANES),
    )
    across = lax.ppermute(own, "rows_0", SWAP)
    sibling = lax.ppermute(own, "rows_1", SWAP)
    one = ((PART_IDS + N_COLS, LANES), F32)
    two = ((PART_IDS + 2 * N_COLS, LANES), F32)
    sent = pltpu.HBM((N_DEV * CAP, EMB), BF16)
    first, send, rest = scored(
        first_kernel,
        2,
        [two],
        [pltpu.VMEM((N_DEV * CAP, EMB), BF16), pltpu.SemaphoreType.DMA((SEND_STEPS + 2,))],
        (queries, pos, own, sibling, slots),
        "score_first",
        [sent, pltpu.HBM((REST_ROWS, EMB), BF16)],
    )
    pool_emb = lax.all_to_all(send, ROWS_COLS, split_axis=0, concat_axis=0, tiled=True)
    far = lax.ppermute(across, "rows_1", SWAP)
    (middle,) = scored(
        next_kernel, 2, [one], [], (queries, pos, rest, across, first), "score_next"
    )
    mine, *to_x = scored(
        last_kernel,
        1,
        [((X_ROWS, LANES), F32)] * N_X,
        [pltpu.VMEM(*one)],
        (queries, pos, far, first, middle),
        "score_last",
    )
    held = [mine] + [
        lax.ppermute(part, "cols_1", [(x, (x + step) % N_X) for x in range(N_X)])
        for step, part in enumerate(to_x, 1)
    ]
    parts = lax.all_to_all(
        collect(held, pool_emb), ("cols_0", "cols_2"), split_axis=0, concat_axis=0, tiled=True
    )
    loss, ids, pool_emb = merge(parts, pool_emb)
    return (pool_emb, ids.reshape(-1), loss.reshape(-1))


def solution(mesh):
    torus = Mesh(
        mesh.devices.reshape(2, 2, 2, 4, 4), ("rows_0", "rows_1", "cols_0", "cols_1", "cols_2")
    )
    placed = (
        P(ROWS_COLS, None),
        P(),
        P(),
        P(ROWS_COLS),
        P(ROWS_COLS),
        P(ROWS_COLS, None),
        P(ROWS, None),
        P(),
    )
    return jax.shard_map(
        local,
        mesh=torus,
        in_specs=placed,
        out_specs=(P(ROWS_COLS, None), P(ROWS_COLS), P(ROWS)),
        check_vma=False,
    )
```
